256 devices in a mesh: pt: 8 (over x, y_lo), tp: 32 (over y_hi, z, core).
Axes of the slice: x: 4, y: 4 (y_hi: 2, y_lo: 2; y = y_hi * 2 + y_lo), z: 8, core: 2. Of those that a mesh axis runs over, the one named last changes fastest.
Arguments:
- tokens: bfloat16 [4096, 4096], P('pt', 'tp'), may hold values from -6 to 6
- t_values: float32 [8], replicated, may hold values from 0.05 to 0.95
- gate_start: bfloat16 [4096, 14336], P('pt', 'tp'), may hold values from -0.09375 to 0.09375
- gate_bend: bfloat16 [4096, 14336], P('pt', 'tp'), may hold values from -0.1875 to 0.1875
- gate_end: bfloat16 [4096, 14336], P('pt', 'tp'), may hold values from -0.09375 to 0.09375
- up_start: bfloat16 [4096, 14336], P('pt', 'tp'), may hold values from -0.09375 to 0.09375
- up_bend: bfloat16 [4096, 14336], P('pt', 'tp'), may hold values from -0.1875 to 0.1875
- up_end: bfloat16 [4096, 14336], P('pt', 'tp'), may hold values from -0.09375 to 0.09375
- hidden_grad: bfloat16 [4096, 14336], P('pt', 'tp'), may hold values from -6 to 6
Outputs:
- hidden: bfloat16 [4096, 14336], P('pt', 'tp')
- input_grad: bfloat16 [4096, 4096], P('pt', 'tp')
- gate_bend_grad: float32 [4096, 14336], P('pt', 'tp')
- up_bend_grad: float32 [4096, 14336], P('pt', 'tp')
The draws below stay inside these ranges and needn't reach their ends.
All inputs are finite; a program needn't handle non-finite values.
Results may differ from the reference program's by a relative error of at most 0.014.
Values may be sent and summed in bfloat16 or wider, within the bound.
A program may use at most 128 MiB of HBM per device.

```python
import jax
import jax.numpy as jnp
from jax import lax

D = 4096
FF = 14336
TOK_PT = 512
POINTS = 8
TOKENS = 4096
N_PT = 8


def spiked(result, stream_key, source, target, parts, factor):
    owner, partner = [(jnp.arange(result.shape[axis_at]) // (result.shape[axis_at] // parts)).reshape([-1 if axis == axis_at else 1 for axis in range(result.ndim)]) for axis_at in (source, target)]
    chosen = jax.random.permutation(stream_key, parts)[partner]
    strong = (owner == chosen) | (owner == (partner + parts // 2) % parts)
    return jnp.where(strong, factor * result, result)


def steps_of(key, extent, split, smallest, top_value):
    def one(axis_at, shards_of):
        heights = jax.random.uniform(jax.random.fold_in(jax.random.fold_in(key, 6), axis_at), (shards_of,), jnp.float32, smallest / len(split), top_value / len(split))
        return jnp.repeat(jnp.exp(heights), extent[axis_at] // shards_of).reshape((-1,) + (1,) * (len(extent) - axis_at - 1))

    loudness = one(*split[0])
    for cut in split[1:]:
        loudness = loudness * one(*cut)
    return loudness


def centred(stream_key, shape, deviation, bound, pieces=(), kind=jnp.bfloat16):
    result = deviation * jax.random.normal(stream_key, shape, jnp.float32)
    if pieces:
        result = result * steps_of(stream_key, shape, pieces, -0.22, 0.18)
    return jnp.clip(result, -bound, bound).astype(kind)


def bell_draw_with(rng, dims, scale, bound, pieces, heavy, held_as=jnp.bfloat16):
    drawn = scale * jax.random.normal(rng, dims, jnp.float32)
    if pieces:
        drawn = drawn * steps_of(rng, dims, pieces, -0.22, 0.18)
    return jnp.clip(spiked(drawn, jax.random.fold_in(rng, 3), *heavy), -bound, bound).astype(held_as)


def setup_inputs(seed: int = 0) -> dict:
    key_of = jax.random.split(jax.random.key(seed), 10)
    tokens = bell_draw_with(key_of[0], (TOKENS, D), 1.0, 6.0, ((0, 8), (1, 32)), (0, 1, 32, 2.75))
    t_values = jnp.clip(jax.random.uniform(key_of[1], (POINTS,), jnp.float32, 0.05, 0.95), 0.05, 0.95)
    gate_start = centred(key_of[2], (D, FF), D ** -0.5, 0.09375, ((0, 8), (1, 32)))
    gate_bend = bell_draw_with(key_of[3], (D, FF), D ** -0.5, 0.1875, ((0, 8), (1, 32)), (1, 0, 32, 2.75))
    gate_end = centred(key_of[4], (D, FF), D ** -0.5, 0.09375, ((0, 8), (1, 32)))
    up_start = centred(key_of[5], (D, FF), D ** -0.5, 0.09375, ((0, 8), (1, 32)))
    up_bend = bell_draw_with(key_of[6], (D, FF), D ** -0.5, 0.1875, ((0, 8), (1, 32)), (1, 0, 32, 2.75))
    up_end = centred(key_of[7], (D, FF), D ** -0.5, 0.09375, ((0, 8), (1, 32)))
    hidden_grad = centred(key_of[8], (TOKENS, FF), 1.0, 6.0, ((0, 8), (1, 32)))
    return dict(tokens=tokens, t_values=t_values, gate_start=gate_start, gate_bend=gate_bend, gate_end=gate_end, up_start=up_start, up_bend=up_bend, up_end=up_end, hidden_grad=hidden_grad)


def blend(first, middle, last, start, bend, end):
    mixed = first * start.astype(jnp.float32) + middle * bend.astype(jnp.float32) + last * end.astype(jnp.float32)
    return mixed.astype(jnp.bfloat16)


def reference(tokens, t_values, gate_start, gate_bend, gate_end, up_start, up_bend, up_end, hidden_grad):
    inputs = tokens.reshape(N_PT, TOK_PT, D)
    grads_in = hidden_grad.reshape(N_PT, TOK_PT, FF)

    def point(carry, item):
        rows, cot, t_here = item
        first = (1.0 - t_here) ** 2
        middle = 2.0 * t_here * (1.0 - t_here)
        last = t_here * t_here
        gate_w = blend(first, middle, last, gate_start, gate_bend, gate_end)
        up_w = blend(first, middle, last, up_start, up_bend, up_end)
        gate = jnp.dot(rows, gate_w, preferred_element_type=jnp.float32)
        up = jnp.dot(rows, up_w, preferred_element_type=jnp.float32)
        sig = jax.nn.sigmoid(gate)
        act = gate * sig
        hidden = (act * up).astype(jnp.bfloat16)
        cotf = cot.astype(jnp.float32)
        d_up = cotf * act
        d_gate = cotf * up * sig * (1.0 + gate * (1.0 - sig))
        input_grad = (jnp.dot(d_gate.astype(jnp.bfloat16), gate_w.T, preferred_element_type=jnp.float32)
                      + jnp.dot(d_up.astype(jnp.bfloat16), up_w.T, preferred_element_type=jnp.float32)).astype(jnp.bfloat16)
        scaled_gate = (middle * d_gate).astype(jnp.bfloat16)
        scaled_up = (middle * d_up).astype(jnp.bfloat16)
        total_gate = carry[0] + jnp.dot(rows.T, scaled_gate, preferred_element_type=jnp.float32)
        total_up = carry[1] + jnp.dot(rows.T, scaled_up, preferred_element_type=jnp.float32)
        return (total_gate, total_up), (hidden, input_grad)

    empty = jnp.zeros((D, FF), jnp.float32)
    sums, outs = lax.scan(point, (empty, empty), (inputs, grads_in, t_values.astype(jnp.float32)))
    hidden = outs[0].reshape(TOKENS, FF)
    input_grad = outs[1].reshape(TOKENS, D)
    return hidden, input_grad, sums[0], sums[1]
```

```python
import functools

import jax
import jax.numpy as jnp
from jax import lax
from jax.experimental import pallas as pl
from jax.experimental.pallas import tpu as pltpu
from jax.sharding import PartitionSpec as P

MESH = pl.DeviceIdType.MESH
F32, BF = jnp.float32, jnp.bfloat16

ROWS = ((0, 256), (256, 256))
COLS = ((0, 256), (256, 256), (512, 256), (768, 128))
CELLS = ((0, 0), (1, 0), (0, 1), (1, 1), (0, 2), (0, 3), (1, 2), (1, 3))
NH, NF, NC = len(ROWS), len(COLS), len(CELLS)
HOPS = ((4, 3), (3, 4))
KORDER = (4, 3, 5, 2, 6, 1, 7, 0)


def div(a, b):
    return lax.div(a, jnp.int32(b))


def rem(a, b):
    return lax.rem(a, jnp.int32(b))


def mul_of(a, b):
    return pl.multiple_of(a, b)


def kernel(
    tok, ts, gs, gb, ge, us, ub, ue, hg,
    hid, ig, gg, ug,
    xbuf, xt, rawp, rawm, wbuf, fbuf, sbuf, r1, r2, dbuf, dwown, ysend, yrecv,
    dxo, dxs, dxr, zs, zr, fs, fr, ta, tb, hgm,
    p0_s, p0_r, tz_s, tz_r, td_s, td_r, w_s, w_r, x_s, x_r, y_s, y_r,
    dd_s, dd_r, dz_s, dz_r, f_s, f_r,
):
    p, t = lax.axis_index("pt"), lax.axis_index("tp")
    x, g = div(p, 2), rem(p, 2)
    yh, z, c = div(t, 16), rem(div(t, 2), 8), rem(t, 2)
    xp, xm, x2 = rem(x + 1, 4), rem(x + 3, 4), rem(x + 2, 4)
    dev_xp, dev_xm = (2 * xp + g, t), (2 * xm + g, t)
    dev_y = (2 * x + (1 - g), t)
    dev_c = (p, yh * 16 + z * 2 + (1 - c))
    dev_z = ((p, yh * 16 + rem(z + 1, 8) * 2 + c), (p, yh * 16 + rem(z + 7, 8) * 2 + c))
    pp, pq = 2 * div(t, 8) + g, 8 * x + rem(t, 8)
    t2 = rem(t + 16, 32)
    dev_p = (pp, pq)
    dev_d2 = (pp, rem(pq + 16, 32))
    dev_s2 = (2 * div(t2, 8) + g, 8 * x + rem(t, 8))
    away = div(t, 8) != x

    barrier = pltpu.get_barrier_semaphore()
    for dev in (dev_xp, dev_xm, dev_y, dev_c, dev_z[0], dev_z[1], dev_d2, dev_s2):
        pl.semaphore_signal(barrier, inc=1, device_id=dev, device_id_type=MESH)

    @pl.when(away)
    def _():
        pl.semaphore_signal(barrier, inc=1, device_id=dev_p, device_id_type=MESH)

    pl.semaphore_wait(barrier, 8 + away.astype(jnp.int32))

    sent = []

    def rc(src, dst, ss, rs, dev):
        return pltpu.make_async_remote_copy(
            src_ref=src, dst_ref=dst, send_sem=ss, recv_sem=rs, device_id=dev, device_id_type=MESH
        )

    def send(src, dst, ss, rs, dev):
        d = rc(src, dst, ss, rs, dev)
        d.start()
        sent.append(d)

    def arrived(dst, ss, rs, dev):
        rc(dst, dst, ss, rs, dev).wait_recv()

    def block(tidx, h):
        r0, rn = ROWS[h]
        row = mul_of(512 * div(tidx, 8) + r0, 32)
        return xbuf.at[pl.ds(row, rn), pl.ds(mul_of(128 * rem(tidx, 8), 128), 128)]

    def tblock(z0, piece, cc, h):
        return block(rem(yh + piece, 2) * 16 + z0 * 2 + cc, h)

    def tok_scatter(h):
        r0, rn = ROWS[h]
        mine = tok.at[pl.ds(r0, rn), :]

        @pl.when(away)
        def _():
            rc(mine, block(pq, h), p0_s.at[h, 0], p0_r.at[h, 0], dev_p).start()

        send(mine, block(pq, h), p0_s.at[h, 1], p0_r.at[h, 1], dev_d2)

        @pl.when(jnp.logical_not(away))
        def _():
            block(t, h)[...] = tok[pl.ds(r0, rn), :]

    def tok_arrive(h, piece):
        if piece == 0:
            @pl.when(away)
            def _():
                arrived(block(t, h), p0_s.at[h, 0], p0_r.at[h, 0], dev_p)
        else:
            arrived(block(t2, h), p0_s.at[h, 1], p0_r.at[h, 1], dev_d2)

    def z_at(direction, s):
        return rem(z + 8 - s, 8) if direction == 0 else rem(z + s, 8)

    def to_sibling(h, piece, direction, s):
        slot = piece * 8 + (s if direction == 0 else (0 if s == 0 else HOPS[0][piece] + s))
        b = tblock(z_at(direction, s), piece, c, h)
        send(b, b, td_s.at[h, slot], td_r.at[h, slot], dev_c)

    def tok_step(h, s):
        for piece in (0, 1):
            if s == 0:
                tok_arrive(h, piece)
            for direction in (0, 1):
                if s > HOPS[direction][piece]:
                    continue
                b = tblock(z_at(direction, s), piece, c, h)
                if s > 0:
                    arrived(b, tz_s.at[h, direction, piece, s - 1], tz_r.at[h, direction, piece, s - 1],
                            dev_z[1 - direction])
                if s < HOPS[direction][piece]:
                    send(b, b, tz_s.at[h, direction, piece, s], tz_r.at[h, direction, piece, s], dev_z[direction])
                if s > 0 or direction == 0:
                    to_sibling(h, piece, direction, s)

    def tok_done(h):
        for piece in (0, 1):
            for direction in (0, 1):
                for s in range(HOPS[direction][piece] + 1):
                    if s == 0 and direction == 1:
                        continue
                    slot = piece * 8 + (s if direction == 0 else HOPS[0][piece] + s)
                    arrived(tblock(z_at(direction, s), piece, 1 - c, h), td_s.at[h, slot], td_r.at[h, slot], dev_c)

    def tok_transpose(h):
        r0, rn = ROWS[h]

        def one(i, _):
            jr, cb = div(i, 8), rem(i, 8)
            v = xbuf[pl.ds(mul_of(512 * jr + r0, 32), rn), pl.ds(mul_of(128 * cb, 128), 128)]
            xt[jr, pl.ds(mul_of(128 * cb, 128), 128), pl.ds(r0, rn)] = v.T
            return 0

        lax.fori_loop(0, 32, one, 0)

    raws = ((gs, us), (gb, ub), (ge, ue))

    def w_send(f):
        for m in range(3):
            if f < 3:
                for k in range(2):
                    i = f * 6 + m * 2 + k
                    send(raws[m][k].at[:, pl.ds(128 * f, 128)], rawp.at[i], w_s.at[i], w_r.at[i], dev_y)
            else:
                i = 18 + m
                send(rawm.at[m], rawp.at[i], w_s.at[i], w_r.at[i], dev_y)

    def w_arrive(f):
        for i in range(f * 6, f * 6 + 6) if f < 3 else range(18, 21):
            arrived(rawp.at[i], w_s.at[i], w_r.at[i], dev_y)

    lane = lax.broadcasted_iota(jnp.int32, (128, 128), 1)

    def pack():
        for m in range(3):
            ta[:, 0:64] = raws[m][0][:, 384:448].astype(F32)
            tb[:, 0:64] = raws[m][1][:, 384:448].astype(F32)

            def one(i, _):
                r = pl.ds(mul_of(i * 128, 128), 128)
                rawm[m, r, :] = jnp.where(lane < 64, ta[r, :], pltpu.roll(tb[r, :], 64, 1)).astype(BF)
                return 0

            lax.fori_loop(0, 4, one, 0)

    ta[...] = jnp.zeros_like(ta)
    tb[...] = jnp.zeros_like(tb)
    hgm[...] = jnp.zeros_like(hgm)
    hgm[:, 0:64] = hg[:, 384:448].astype(F32)

    tv = [ts[2 * j + g] for j in range(4)]
    coef = [((1.0 - v) * (1.0 - v), 2.0 * v * (1.0 - v), v * v) for v in tv]

    def blend(f, own):
        side = g if own else 1 - g

        def one(i, _):
            r = pl.ds(mul_of(i * 64, 64), 64)
            w = pl.ds(mul_of(side * 512 + i * 64, 64), 64)
            for k in range(2 if f < 3 else 1):
                if f < 3:
                    v = [(raws[m][k][r, 128 * f:128 * f + 128] if own else rawp[f * 6 + m * 2 + k, r, :])
                         for m in range(3)]
                else:
                    v = [(rawm[m, r, :] if own else rawp[18 + m, r, :]) for m in range(3)]
                v = [a.astype(F32) for a in v]
                c0 = COLS[f][0] + 128 * k
                for j in range(4):
                    b0, b1, b2 = coef[j]
                    wbuf[j, w, c0:c0 + 128] = (b0 * v[0] + b1 * v[1] + b2 * v[2]).astype(BF)
            return 0

        lax.fori_loop(0, 8, one, 0)

    def cell(i):
        h, f = CELLS[i]
        return ROWS[h] + COLS[f] + (f,)

    def at(ref, i, lo=0.0, hi=1.0):
        r0, rn, c0, cn, _ = cell(i)
        return ref.at[pl.ds(r0 + int(rn * lo), int(rn * (hi - lo))), pl.ds(c0, cn)]

    def forward(i):
        r0, rn, c0, cn, _ = cell(i)

        def one(k, _):
            jr = rem(x + k, 4)
            fbuf[k, r0:r0 + rn, c0:c0 + cn] = jnp.dot(
                xbuf[pl.ds(mul_of(512 * jr + r0, 32), rn), :], wbuf[jr, :, c0:c0 + cn],
                preferred_element_type=F32)
            return 0

        lax.fori_loop(0, 4, one, 0)
        sbuf[0, r0:r0 + rn, c0:c0 + cn] = fbuf[2, r0:r0 + rn, c0:c0 + cn].astype(BF)
        send(at(sbuf.at[0], i, 0.0, 0.5), at(r1, i, 0.0, 0.5), x_s.at[i, 0], x_r.at[i, 0], dev_xp)
        send(at(sbuf.at[0], i, 0.5, 1.0), at(r1, i, 0.5, 1.0), x_s.at[i, 1], x_r.at[i, 1], dev_xm)

    def reduce(i):
        r0, rn, c0, cn, _ = cell(i)
        n = rn // 2
        a, b, cs = slice(r0, r0 + n), slice(r0 + n, r0 + rn), slice(c0, c0 + cn)
        arrived(at(r1, i, 0.0, 0.5), x_s.at[i, 0], x_r.at[i, 0], dev_xm)
        sbuf[1, a, cs] = (fbuf[1, a, cs] + r1[a, cs].astype(F32)).astype(BF)
        sbuf[1, b, cs] = fbuf[1, b, cs].astype(BF)
        send(at(sbuf.at[1], i), at(r2.at[0], i), x_s.at[i, 2], x_r.at[i, 2], dev_xp)
        arrived(at(r1, i, 0.5, 1.0), x_s.at[i, 1], x_r.at[i, 1], dev_xp)
        sbuf[2, a, cs] = fbuf[3, a, cs].astype(BF)
        sbuf[2, b, cs] = (fbuf[3, b, cs] + r1[b, cs].astype(F32)).astype(BF)
        send(at(sbuf.at[2], i), at(r2.at[1], i), x_s.at[i, 3], x_r.at[i, 3], dev_xm)

    def middle(i):
        r0, rn, c0, cn, f = cell(i)
        arrived(at(r2.at[0], i), x_s.at[i, 2], x_r.at[i, 2], dev_xm)
        arrived(at(r2.at[1], i), x_s.at[i, 3], x_r.at[i, 3], dev_xp)

        def total(r, lo):
            cs = pl.ds(lo, 128)
            return fbuf[0, r, cs] + r2[0, r, cs].astype(F32) + r2[1, r, cs].astype(F32)

        def one(k, _):
            r = pl.ds(mul_of(r0 + k * 32, 32), 32)
            if f < 3:
                gate, up = total(r, c0), total(r, c0 + 128)
                cot = hg[r, 128 * f:128 * f + 128].astype(F32)
            else:
                gate = total(r, c0)
                up = pltpu.roll(gate, 64, 1)
                cot = hgm[r, :]
            sig = jax.nn.sigmoid(gate)
            act = gate * sig
            hidden = (act * up).astype(BF)
            du = cot * act
            dg = cot * up * sig * (1.0 + gate * (1.0 - sig))
            if f < 3:
                hid[r, 128 * f:128 * f + 128] = hidden
                dbuf[x, r, c0:c0 + 128] = dg.astype(BF)
                dbuf[x, r, c0 + 128:c0 + 256] = du.astype(BF)
            else:
                hid[r, 384:448] = hidden[:, 0:64]
                dbuf[x, r, c0:c0 + 128] = jnp.where(lane[0:32] < 64, dg, pltpu.roll(du, 64, 1)).astype(BF)
            return 0

        lax.fori_loop(0, rn // 32, one, 0)
        send(at(dbuf.at[x], i), at(dbuf.at[x], i), x_s.at[i, 4], x_r.at[i, 4], dev_xp)
        send(at(dbuf.at[x], i), at(dbuf.at[x], i), x_s.at[i, 5], x_r.at[i, 5], dev_xm)

    def spread(i):
        arrived(at(dbuf.at[xm], i), x_s.at[i, 4], x_r.at[i, 4], dev_xm)
        b = at(dbuf.at[xm], i, 0.0, 0.5)
        send(b, b, x_s.at[i, 6], x_r.at[i, 6], dev_xp)
        arrived(at(dbuf.at[xp], i), x_s.at[i, 5], x_r.at[i, 5], dev_xp)
        b = at(dbuf.at[xp], i, 0.5, 1.0)
        send(b, b, x_s.at[i, 7], x_r.at[i, 7], dev_xm)

    def gathered(i):
        arrived(at(dbuf.at[x2], i, 0.0, 0.5), x_s.at[i, 6], x_r.at[i, 6], dev_xm)
        arrived(at(dbuf.at[x2], i, 0.5, 1.0), x_s.at[i, 7], x_r.at[i, 7], dev_xp)

    def bend(f):
        c0, cn = COLS[f]

        def part(row):
            acc = None
            for j in range(4):
                d = coef[j][1] * jnp.dot(xt[j, pl.ds(row, 256), :], dbuf[j, :, c0:c0 + cn],
                                         preferred_element_type=F32)
                acc = d if acc is None else acc + d
            return acc

        def one(k, _):
            q = rem(k, 2)
            mine = part(mul_of(rem(1 - g + div(k, 2), 2) * 512 + q * 256, 256))
            r = pl.ds(mul_of(q * 256, 256), 256)

            @pl.when(k < 2)
            def _():
                ysend[r, c0:c0 + cn] = mine.astype(BF)

            @pl.when(k >= 2)
            def _():
                dwown[r, c0:c0 + cn] = mine
            return 0

        lax.fori_loop(0, 4, one, 0)
        s = (slice(None), pl.ds(c0, cn))
        send(ysend.at[s], yrecv.at[s], y_s.at[f], y_r.at[f], dev_y)

    def bend_out(f):
        c0, cn = COLS[f]
        arrived(yrecv.at[:, pl.ds(c0, cn)], y_s.at[f], y_r.at[f], dev_y)

        def one(k, _):
            r = pl.ds(mul_of(k * 64, 64), 64)
            v = dwown[r, c0:c0 + cn] + yrecv[r, c0:c0 + cn].astype(F32)
            if f < 3:
                gg[r, 128 * f:128 * f + 128] = v[:, 0:128]
                ug[r, 128 * f:128 * f + 128] = v[:, 128:256]
            else:
                gg[r, 384:448] = v[:, 0:64]
                ug[r, 384:448] = pltpu.roll(v, 64, 1)[:, 0:64]
            return 0

        lax.fori_loop(0, 8, one, 0)

    def back(h):
        r0, rn = ROWS[h]

        def one(i, _):
            piece, q = rem(i, 2), div(i, 2)
            k = rem(4 + div(q + 1, 2) * (1 - 2 * rem(q, 2)) + 8, 8)
            zd, yd = rem(z + k, 8), rem(yh + piece, 2)
            jr = yd * 2 + div(zd, 4)
            v = lax.dot_general(
                dbuf[jr, r0:r0 + rn, :], wbuf[jr, pl.ds(mul_of(256 * rem(zd, 4), 256), 256), :],
                (((1,), (1,)), ((), ())), preferred_element_type=F32)
            s = piece * 8 + k
            dxo[s, r0:r0 + rn, :] = jnp.where(c == 0, v[:, 0:128], v[:, 128:256])
            dxs[s, r0:r0 + rn, :] = jnp.where(c == 0, v[:, 128:256], v[:, 0:128]).astype(BF)
            rc(dxs.at[s, pl.ds(r0, rn), :], dxr.at[s, pl.ds(r0, rn), :], dd_s.at[h, s], dd_r.at[h, s], dev_c).start()
            return 0

        lax.fori_loop(0, 16, one, 0)

    def core_sum(h, piece, k):
        r0, rn = ROWS[h]
        s = piece * 8 + k
        arrived(dxr.at[s, pl.ds(r0, rn), :], dd_s.at[h, s], dd_r.at[h, s], dev_c)
        return dxo[s, r0:r0 + rn, :] + dxr[s, r0:r0 + rn, :].astype(F32)

    def zslot(direction, piece, s):
        return (direction * 2 + piece) * 4 + s

    def back_step(h, s):
        r0, rn = ROWS[h]
        for piece in (0, 1):
            for direction in (0, 1):
                first = 4 - HOPS[direction][piece]
                if s < first:
                    continue
                k = 4 - s if direction == 0 else (8 - (4 - s)) % 8
                v = core_sum(h, piece, k)
                if s > first:
                    i = zslot(direction, piece, s - 1)
                    arrived(zr.at[i, pl.ds(r0, rn), :], dz_s.at[h, i], dz_r.at[h, i], dev_z[1 - direction])
                    v = v + zr[i, r0:r0 + rn, :].astype(F32)
                i = zslot(direction, piece, s)
                zs[i, r0:r0 + rn, :] = v.astype(BF)
                send(zs.at[i, pl.ds(r0, rn), :], zr.at[i, pl.ds(r0, rn), :], dz_s.at[h, i], dz_r.at[h, i],
                     dev_z[direction])

    def back_last(h):
        r0, rn = ROWS[h]
        rows = pl.ds(r0, rn)
        for piece in (0, 1):
            v = core_sum(h, piece, 0)
            for direction in (0, 1):
                i = zslot(direction, piece, 3)
                arrived(zr.at[i, rows, :], dz_s.at[h, i], dz_r.at[h, i], dev_z[1 - direction])
                v = v + zr[i, r0:r0 + rn, :].astype(F32)
            fs[piece, r0:r0 + rn, :] = v.astype(BF)
            if piece == 0:
                @pl.when(away)
                def _():
                    rc(fs.at[0, rows, :], fr.at[0, rows, :], f_s.at[h, 0], f_r.at[h, 0], dev_p).start()

                @pl.when(jnp.logical_not(away))
                def _():
                    fr[0, r0:r0 + rn, :] = fs[0, r0:r0 + rn, :]
            else:
                send(fs.at[1, rows, :], fr.at[1, rows, :], f_s.at[h, 1], f_r.at[h, 1], dev_s2)

    def back_out(h):
        r0, rn = ROWS[h]
        rows = pl.ds(r0, rn)

        @pl.when(away)
        def _():
            arrived(fr.at[0, rows, :], f_s.at[h, 0], f_r.at[h, 0], dev_p)

        arrived(fr.at[1, rows, :], f_s.at[h, 1], f_r.at[h, 1], dev_d2)
        ig[r0:r0 + rn, :] = (fr[0, r0:r0 + rn, :].astype(F32) + fr[1, r0:r0 + rn, :].astype(F32)).astype(BF)

    for h in range(NH):
        tok_scatter(h)
    for f in range(3):
        w_send(f)
    pack()
    w_send(3)
    for f in range(NF):
        blend(f, True)
    for s in range(5):
        for h in range(NH):
            tok_step(h, s)
    for h in range(NH):
        tok_done(h)
        tok_transpose(h)

    blended = set()

    def ready(i):
        f = CELLS[i][1]
        if f not in blended:
            w_arrive(f)
            blend(f, False)
            blended.add(f)

    left_f = {f: sum(1 for a in CELLS if a[1] == f) for f in range(NF)}
    left_h = {h: sum(1 for a in CELLS if a[0] == h) for h in range(NH)}
    queue = []

    def finish(i):
        h, f = CELLS[i]
        gathered(i)
        left_f[f] -= 1
        left_h[h] -= 1
        if left_h[h] == 0:
            back(h)
            queue.extend([functools.partial(back_step, h, s) for s in range(4)]
                         + [functools.partial(back_last, h), functools.partial(back_out, h)])
        if left_f[f] == 0:
            if queue:
                queue.pop(0)()
            bend(f)

    def step_back(last):
        if queue and not last:
            queue.pop(0)()

    for n in range(NC + 2):
        if n < NC:
            ready(n)
            forward(n)
        if 1 <= n <= NC:
            middle(n - 1)
        step_back(n >= NC)
        if n < NC:
            reduce(n)
        if 1 <= n <= NC:
            spread(n - 1)
        step_back(n >= NC)
        if n >= 2:
            finish(n - 2)
    outs = list(range(NF))
    while queue:
        queue.pop(0)()
        if outs:
            bend_out(outs.pop(0))
    while outs:
        bend_out(outs.pop(0))

    for d in sent:
        d.wait_send()
    for h in range(NH):
        r0, rn = ROWS[h]

        @pl.when(away)
        def _():
            rc(tok.at[pl.ds(r0, rn), :], block(pq, h), p0_s.at[h, 0], p0_r.at[h, 0], dev_p).wait_send()
            rc(fs.at[0, pl.ds(r0, rn), :], fr.at[0, pl.ds(r0, rn), :], f_s.at[h, 0], f_r.at[h, 0], dev_p).wait_send()

        def drain(s, _):
            rc(dxs.at[s, pl.ds(r0, rn), :], dxr.at[s, pl.ds(r0, rn), :], dd_s.at[h, s], dd_r.at[h, s],
               dev_c).wait_send()
            return 0

        lax.fori_loop(0, 16, drain, 0)


def per_device(tokens, t_values, *rest):
    v = pl.BlockSpec(memory_space=pltpu.VMEM)
    dma = pltpu.SemaphoreType.DMA
    scratch = [
        pltpu.VMEM((2048, 1024), BF),
        pltpu.VMEM((4, 1024, 512), BF),
        pltpu.VMEM((21, 512, 128), BF),
        pltpu.VMEM((3, 512, 128), BF),
        pltpu.VMEM((4, 1024, 896), BF),
        pltpu.VMEM((4, 512, 896), F32),
        pltpu.VMEM((3, 512, 896), BF),
        pltpu.VMEM((512, 896), BF),
        pltpu.VMEM((2, 512, 896), BF),
        pltpu.VMEM((4, 512, 896), BF),
        pltpu.VMEM((512, 896), F32),
        pltpu.VMEM((512, 896), BF),
        pltpu.VMEM((512, 896), BF),
        pltpu.VMEM((16, 512, 128), F32),
        pltpu.VMEM((16, 512, 128), BF),
        pltpu.VMEM((16, 512, 128), BF),
        pltpu.VMEM((16, 512, 128), BF),
        pltpu.VMEM((16, 512, 128), BF),
        pltpu.VMEM((2, 512, 128), BF),
        pltpu.VMEM((2, 512, 128), BF),
        pltpu.VMEM((512, 128), F32),
        pltpu.VMEM((512, 128), F32),
        pltpu.VMEM((512, 128), F32),
    ]
    for shape in ((NH, 2), (NH, 2, 2, 4), (NH, 16), (21,), (NC, 8), (NF,), (NH, 16), (NH, 16), (NH, 2)):
        scratch += [dma(shape), dma(shape)]
    return tuple(
        pl.pallas_call(
            kernel,
            out_shape=(
                jax.ShapeDtypeStruct((512, 448), BF),
                jax.ShapeDtypeStruct((512, 128), BF),
                jax.ShapeDtypeStruct((512, 448), F32),
                jax.ShapeDtypeStruct((512, 448), F32),
            ),
            in_specs=[v, pl.BlockSpec(memory_space=pltpu.SMEM)] + [v] * 7,
            out_specs=(v, v, v, v),
            scratch_shapes=scratch,
            compiler_params=pltpu.CompilerParams(
                collective_id=0, has_side_effects=True, vmem_limit_bytes=66_000_000
            ),
        )(tokens, t_values, *rest)
    )


def solution(mesh):
    return jax.shard_map(
        per_device,
        mesh=mesh,
        in_specs=(P("pt", "tp"), P()) + (P("pt", "tp"),) * 7,
        out_specs=(P("pt", "tp"),) * 4,
        check_vma=False,
    )
```

```python
import jax
import jax.numpy as jnp
from jax import lax
from jax.experimental import pallas as pl
from jax.experimental.pallas import tpu as pltpu
from jax.sharding import PartitionSpec as P

MESH = pl.DeviceIdType.MESH
F32, BF = jnp.float32, jnp.bfloat16

TOKS = ((0, 256), (256, 256))
UNITS = ((0, 256), (256, 256), (512, 256), (768, 128))
CELLS = ((0, 0), (1, 0), (0, 1), (1, 1), (0, 2), (0, 3), (1, 2), (1, 3))
NH, NF, NC = len(TOKS), len(UNITS), len(CELLS)
HOPS = ((4, 3), (3, 4))


def div(a, b):
    return lax.div(a, jnp.int32(b))


def rem(a, b):
    return lax.rem(a, jnp.int32(b))


def mul_of(a, b):
    return pl.multiple_of(a, b)


def kernel(
    tok_in, ts_in, gs, gb, ge, us, ub, ue, hg_in,
    hid_out, ig_out, gg_out, ug_out,
    ts, tok, tokt, raw, rawp, hg, hid, ig, xt, xb, wbuf, fbuf, sbuf, r1, r2, dbuf, dn, dw, ysend, yrecv,
    dxo, dxs, dxr, zs, zr, fs, fr,
    l_s, o_s,
    p0_s, p0_r, tz_s, tz_r, td_s, td_r, w_s, w_r, x_s, x_r, y_s, y_r,
    dd_s, dd_r, dz_s, dz_r, f_s, f_r,
):
    p, t = lax.axis_index("pt"), lax.axis_index("tp")
    x, g = div(p, 2), rem(p, 2)
    yh, z, c = div(t, 16), rem(div(t, 2), 8), rem(t, 2)
    xp, xm, x2 = rem(x + 1, 4), rem(x + 3, 4), rem(x + 2, 4)
    dev_xp, dev_xm = (2 * xp + g, t), (2 * xm + g, t)
    dev_y = (2 * x + (1 - g), t)
    dev_c = (p, yh * 16 + z * 2 + (1 - c))
    dev_z = ((p, yh * 16 + rem(z + 1, 8) * 2 + c), (p, yh * 16 + rem(z + 7, 8) * 2 + c))
    mirror = div(z, 4) != rem(x, 2)
    zq = jnp.where(mirror, 7 - z, z)
    pp, pq = 2 * div(t, 8) + g, div(x, 2) * 16 + zq * 2 + c
    t2 = rem(t + 16, 32)
    dev_p = (pp, pq)
    dev_d2 = (pp, rem(pq + 16, 32))
    dev_s2 = (2 * div(t2, 8) + g, pq)
    away = div(t, 8) != x

    def column(z0):
        return jnp.where(div(z0, 4) != rem(x, 2), 3 - rem(z0, 4), rem(z0, 4))

    mats = ((gs, us), (gb, ub), (ge, ue))

    def units(f):
        c0, cn = UNITS[f]
        return c0, cn, c0 // 2, cn // 2

    tok_load = pltpu.make_async_copy(tok_in, tok, l_s.at[0])
    hg_load = pltpu.make_async_copy(hg_in, hg, l_s.at[1])
    ts_load = pltpu.make_async_copy(ts_in, ts, l_s.at[2])
    tok_load.start()
    for f in range(NF):
        c0, _, u0, un = units(f)
        for m in range(3):
            for k in range(2):
                pltpu.make_async_copy(
                    mats[m][k].at[pl.ds(u0, un), :], raw.at[m, pl.ds(c0 + k * un, un), :], l_s.at[3 + f]).start()
    ts_load.start()
    hg_load.start()

    barrier = pltpu.get_barrier_semaphore()
    for dev in (dev_xp, dev_xm, dev_y, dev_c, dev_z[0], dev_z[1], dev_d2, dev_s2):
        pl.semaphore_signal(barrier, inc=1, device_id=dev, device_id_type=MESH)

    @pl.when(away)
    def _():
        pl.semaphore_signal(barrier, inc=1, device_id=dev_p, device_id_type=MESH)

    tok_load.wait()
    tokt[...] = tok[...].T
    pl.semaphore_wait(barrier, 8 + away.astype(jnp.int32))

    def rc(src, dst, ss, rs, dev):
        return pltpu.make_async_remote_copy(
            src_ref=src, dst_ref=dst, send_sem=ss, recv_sem=rs, device_id=dev, device_id_type=MESH
        )

    def send(src, dst, ss, rs, dev):
        rc(src, dst, ss, rs, dev).start()

    def arrived(dst, ss, rs, dev):
        rc(dst, dst, ss, rs, dev).wait_recv()

    def left(src, ss, rs, dev):
        rc(src, src, ss, rs, dev).wait_send()

    def block(tidx, h):
        r0, rn = TOKS[h]
        return xt.at[tidx[0], pl.ds(mul_of(128 * tidx[1], 128), 128), pl.ds(r0, rn)]

    def tblock(z0, piece, cc, h):
        return block((rem(yh + piece, 2) * 2 + div(z0, 4), column(z0) * 2 + cc), h)

    there = (x, rem(t, 8))

    def tok_scatter(h):
        r0, rn = TOKS[h]
        mine = tokt.at[:, pl.ds(r0, rn)]

        @pl.when(away)
        def _():
            send(mine, block(there, h), p0_s.at[0], p0_r.at[h, 0], dev_p)

        send(mine, block(there, h), p0_s.at[1], p0_r.at[h, 1], dev_d2)

        @pl.when(jnp.logical_not(away))
        def _():
            block(there, h)[...] = tokt[:, pl.ds(r0, rn)]

    def tok_arrive(h, piece):
        b = tblock(z, piece, c, h)
        if piece == 0:
            @pl.when(away)
            def _():
                arrived(b, p0_s.at[0], p0_r.at[h, 0], dev_p)
        else:
            arrived(b, p0_s.at[1], p0_r.at[h, 1], dev_d2)

    def z_at(direction, s):
        return rem(z + 8 - s, 8) if direction == 0 else rem(z + s, 8)

    def ring_wait(h, s, piece):
        r0, rn = TOKS[h]
        n = sum(s < HOPS[d][piece] for d in (0, 1))
        arrived(zr.at[pl.ds(0, n), pl.ds(0, rn), :], tz_s.at[h], tz_r.at[h, s, piece], dev_z[0])

    def tok_step(h, s):
        for piece in (0, 1):
            if s == 0:
                tok_arrive(h, piece)
            elif s <= max(HOPS[0][piece], HOPS[1][piece]):
                ring_wait(h, s - 1, piece)
            for direction in (0, 1):
                if s < HOPS[direction][piece]:
                    b = tblock(z_at(direction, s), piece, c, h)
                    send(b, b, tz_s.at[h], tz_r.at[h, s, piece], dev_z[direction])
            for direction in (0, 1):
                if s <= HOPS[direction][piece] and (s > 0 or direction == 0):
                    b = tblock(z_at(direction, s), piece, c, h)
                    send(b, b, td_s.at[h], td_r.at[h], dev_c)

    def tok_done(h):
        r0, rn = TOKS[h]
        arrived(xt.at[:, pl.ds(0, 512), pl.ds(r0, rn)], td_s.at[h], td_r.at[h], dev_c)

    def tok_turn(h):
        r0, rn = TOKS[h]

        def one(i, _):
            jr, cb = div(i, 8), rem(i, 8)
            d = pl.ds(mul_of(128 * cb, 128), 128)
            xb[jr, r0:r0 + rn, d] = xt[jr, d, r0:r0 + rn].T
            return 0

        lax.fori_loop(0, 32, one, 0)

    def w_send(f):
        c0, cn = UNITS[f]
        b = raw.at[:, pl.ds(c0, cn), :]
        pltpu.make_async_copy(b, b, l_s.at[3 + f]).wait()
        send(b, rawp.at[:, pl.ds(c0, cn), :], w_s.at[0], w_r.at[f], dev_y)

    def w_arrive(f):
        c0, cn = UNITS[f]
        arrived(rawp.at[:, pl.ds(c0, cn), :], w_s.at[0], w_r.at[f], dev_y)

    ts_load.wait()
    tv = [ts[2 * j + g] for j in range(4)]
    coef = [((1.0 - v) * (1.0 - v), 2.0 * v * (1.0 - v), v * v) for v in tv]

    def blend(f, own):
        c0, cn = UNITS[f]
        src, side = (raw, g) if own else (rawp, 1 - g)
        lanes = pl.ds(mul_of(side * 512, 512), 512)

        def one(i, _):
            r = pl.ds(mul_of(c0 + i * 16, 16), 16)
            v = [src[m, r, :].astype(F32) for m in range(3)]
            for j in range(4):
                b0, b1, b2 = coef[j]
                wbuf[j, r, lanes] = (b0 * v[0] + b1 * v[1] + b2 * v[2]).astype(BF)
            return 0

        lax.fori_loop(0, cn // 16, one, 0)

    def cell(i):
        h, f = CELLS[i]
        return TOKS[h] + UNITS[f] + (f,)

    def at(ref, i, half=None):
        r0, rn, c0, cn, _ = cell(i)
        if half is not None:
            c0, cn = c0 + half * (cn // 2), cn // 2
        return ref.at[pl.ds(c0, cn), pl.ds(r0, rn)]

    def forward(i):
        r0, rn, c0, cn, _ = cell(i)

        def one(k, _):
            for q in (2 * k, 2 * k + 1):
                jr = rem(x + q, 4)
                fbuf[q, c0:c0 + cn, r0:r0 + rn] = jnp.dot(
                    wbuf[jr, c0:c0 + cn, :], xt[jr, :, r0:r0 + rn], preferred_element_type=F32)
            return 0

        lax.fori_loop(0, 2, one, 0)
        sbuf[0, c0:c0 + cn, r0:r0 + rn] = fbuf[2, c0:c0 + cn, r0:r0 + rn].astype(BF)
        send(at(sbuf.at[0], i, 0), at(r1, i, 0), x_s.at[0], x_r.at[i, 0], dev_xp)
        send(at(sbuf.at[0], i, 1), at(r1, i, 1), x_s.at[0], x_r.at[i, 0], dev_xm)

    def reduce(i):
        r0, rn, c0, cn, _ = cell(i)
        n = cn // 2
        a, b, cs = slice(c0, c0 + n), slice(c0 + n, c0 + cn), slice(r0, r0 + rn)
        arrived(at(r1, i), x_s.at[0], x_r.at[i, 0], dev_xm)
        sbuf[1, a, cs] = (fbuf[1, a, cs] + r1[a, cs].astype(F32)).astype(BF)
        sbuf[1, b, cs] = fbuf[1, b, cs].astype(BF)
        send(at(sbuf.at[1], i), at(r2.at[0], i), x_s.at[0], x_r.at[i, 1], dev_xp)
        sbuf[2, a, cs] = fbuf[3, a, cs].astype(BF)
        sbuf[2, b, cs] = (fbuf[3, b, cs] + r1[b, cs].astype(F32)).astype(BF)
        send(at(sbuf.at[2], i), at(r2.at[1], i), x_s.at[0], x_r.at[i, 1], dev_xm)

    def two(i):
        r0, rn, c0, cn, _ = cell(i)
        return r2.at[:, pl.ds(c0, cn), pl.ds(r0, rn)]

    def middle(i):
        r0, rn, c0, cn, f = cell(i)
        arrived(two(i), x_s.at[0], x_r.at[i, 1], dev_xm)
        cs = slice(r0, r0 + rn)

        def total(r):
            return fbuf[0, r, cs] + r2[0, r, cs].astype(F32) + r2[1, r, cs].astype(F32)

        def one(k, _):
            rg = pl.ds(mul_of(c0 + k * 16, 16), 16)
            ru = pl.ds(mul_of(c0 + cn // 2 + k * 16, 16), 16)
            rh = pl.ds(mul_of(c0 // 2 + k * 16, 16), 16)
            gate, up = total(rg), total(ru)
            cot = hg[rh, cs].astype(F32)
            sig = jax.nn.sigmoid(gate)
            act = gate * sig
            hid[rh, cs] = (act * up).astype(BF)
            dbuf[x, rg, cs] = (cot * up * sig * (1.0 + gate * (1.0 - sig))).astype(BF)
            dbuf[x, ru, cs] = (cot * act).astype(BF)
            return 0

        lax.fori_loop(0, cn // 32, one, 0)
        send(at(dbuf.at[x], i), at(dbuf.at[x], i), x_s.at[0], x_r.at[i, 2], dev_xp)
        send(at(dbuf.at[x], i), at(dbuf.at[x], i), x_s.at[0], x_r.at[i, 2], dev_xm)

    def spread(i):
        arrived(two(i), x_s.at[0], x_r.at[i, 2], dev_xm)
        b = at(dbuf.at[xm], i, 0)
        send(b, b, x_s.at[0], x_r.at[i, 3], dev_xp)
        b = at(dbuf.at[xp], i, 1)
        send(b, b, x_s.at[0], x_r.at[i, 3], dev_xm)

    def gathered(i):
        arrived(at(r1, i), x_s.at[0], x_r.at[i, 3], dev_xm)

    def turn(i):
        r0, rn, c0, cn, _ = cell(i)

        def one(j, _):
            dn[j, r0:r0 + rn, c0:c0 + cn] = dbuf[j, c0:c0 + cn, r0:r0 + rn].T
            return 0

        lax.fori_loop(0, 4, one, 0)

    def bend(f):
        c0, cn = UNITS[f]

        def part(lanes):
            acc = None
            for j in range(4):
                d = coef[j][1] * jnp.dot(dbuf[j, c0:c0 + cn, :], xb[j, :, lanes], preferred_element_type=F32)
                acc = d if acc is None else acc + d
            return acc

        def one(k, _):
            q = rem(k, 2)
            mine = part(pl.ds(mul_of(rem(1 - g + div(k, 2), 2) * 512 + q * 256, 256), 256))
            r = pl.ds(mul_of(q * 256, 256), 256)

            @pl.when(k < 2)
            def _():
                ysend[c0:c0 + cn, r] = mine.astype(BF)

            @pl.when(k >= 2)
            def _():
                dw[c0:c0 + cn, r] = mine
            return 0

        lax.fori_loop(0, 4, one, 0)
        send(ysend.at[pl.ds(c0, cn), :], yrecv.at[pl.ds(c0, cn), :], y_s.at[0], y_r.at[f], dev_y)

    def dw_out(f, k):
        c0, _, u0, un = units(f)
        return pltpu.make_async_copy(
            dw.at[pl.ds(c0 + k * un, un), :], (gg_out, ug_out)[k].at[pl.ds(u0, un), :], o_s.at[2])

    hid_copy = pltpu.make_async_copy(hid, hid_out, o_s.at[0])
    ig_copy = pltpu.make_async_copy(ig, ig_out, o_s.at[1])

    def bend_out(f):
        c0, cn = UNITS[f]
        arrived(yrecv.at[pl.ds(c0, cn), :], y_s.at[0], y_r.at[f], dev_y)

        def one(k, _):
            r = pl.ds(mul_of(c0 + k * 32, 32), 32)
            dw[r, :] = dw[r, :] + yrecv[r, :].astype(F32)
            return 0

        lax.fori_loop(0, cn // 32, one, 0)
        dw_out(f, 0).start()
        dw_out(f, 1).start()

    def back(h, part):
        r0, rn = TOKS[h]
        rows = pl.ds(r0, rn)

        def one(piece, _):
            for k in ((4,), (3, 5), (2, 6), (1, 7), (0,))[part]:
                zd, yd = rem(z + k, 8), rem(yh + piece, 2)
                jr = yd * 2 + div(zd, 4)
                v = jnp.dot(dn[jr, r0:r0 + rn, :], wbuf[jr, :, pl.ds(mul_of(256 * column(zd), 256), 256)],
                            preferred_element_type=F32)
                s = k * 2 + piece
                dxo[s, r0:r0 + rn, :] = jnp.where(c == 0, v[:, 0:128], v[:, 128:256])
                dxs[s, r0:r0 + rn, :] = jnp.where(c == 0, v[:, 128:256], v[:, 0:128]).astype(BF)
                send(dxs.at[s, rows, :], dxr.at[s, rows, :], dd_s.at[h], dd_r.at[h, part], dev_c)
            return 0

        lax.fori_loop(0, 2, one, 0)

    def core_sum(h, piece, k):
        r0, rn = TOKS[h]
        s = k * 2 + piece
        return dxo[s, r0:r0 + rn, :] + dxr[s, r0:r0 + rn, :].astype(F32)

    def core_wait(h, part):
        r0, rn = TOKS[h]
        n = 2 if part in (0, 4) else 4
        arrived(dxr.at[pl.ds(0, n), pl.ds(r0, rn), :], dd_s.at[h], dd_r.at[h, part], dev_c)

    def zslot(direction, piece, s):
        return (direction * 2 + piece) * 4 + s

    def back_wait(h, s, piece):
        r0, rn = TOKS[h]
        n = sum(s >= 4 - HOPS[d][piece] for d in (0, 1))
        arrived(zr.at[pl.ds(0, n), pl.ds(r0, rn), :], dz_s.at[h], dz_r.at[h, s, piece], dev_z[0])

    def back_step(h, s):
        r0, rn = TOKS[h]
        core_wait(h, s)
        for piece in (0, 1):
            if s > 4 - max(HOPS[0][piece], HOPS[1][piece]):
                back_wait(h, s - 1, piece)
            for direction in (0, 1):
                first = 4 - HOPS[direction][piece]
                if s < first:
                    continue
                k = 4 - s if direction == 0 else 4 + s
                v = core_sum(h, piece, k)
                if s > first:
                    v = v + zr[zslot(direction, piece, s - 1), r0:r0 + rn, :].astype(F32)
                i = zslot(direction, piece, s)
                zs[i, r0:r0 + rn, :] = v.astype(BF)
                send(zs.at[i, pl.ds(r0, rn), :], zr.at[i, pl.ds(r0, rn), :], dz_s.at[h], dz_r.at[h, s, piece],
                     dev_z[direction])

    def back_last(h):
        r0, rn = TOKS[h]
        rows = pl.ds(r0, rn)
        core_wait(h, 4)
        for piece in (0, 1):
            back_wait(h, 3, piece)
            v = core_sum(h, piece, 0)
            for direction in (0, 1):
                v = v + zr[zslot(direction, piece, 3), r0:r0 + rn, :].astype(F32)
            fs[piece, r0:r0 + rn, :] = v.astype(BF)
            if piece == 0:
                @pl.when(away)
                def _():
                    send(fs.at[0, rows, :], fr.at[0, rows, :], f_s.at[0], f_r.at[h, 0], dev_p)

                @pl.when(jnp.logical_not(away))
                def _():
                    fr[0, r0:r0 + rn, :] = fs[0, r0:r0 + rn, :]
            else:
                send(fs.at[1, rows, :], fr.at[1, rows, :], f_s.at[1], f_r.at[h, 1], dev_s2)

    def back_out(h):
        r0, rn = TOKS[h]
        rows = pl.ds(r0, rn)

        @pl.when(away)
        def _():
            arrived(fr.at[0, rows, :], f_s.at[0], f_r.at[h, 0], dev_p)

        arrived(fr.at[1, rows, :], f_s.at[1], f_r.at[h, 1], dev_d2)
        ig[r0:r0 + rn, :] = (fr[0, r0:r0 + rn, :].astype(F32) + fr[1, r0:r0 + rn, :].astype(F32)).astype(BF)

    for h in range(NH):
        tok_scatter(h)
    for f in range(NF):
        w_send(f)
    for f in range(NF):
        blend(f, True)
    hg_load.wait()
    for h, s in ((0, 0), (1, 0), (0, 1), (0, 2), (1, 1), (0, 3), (1, 2), (0, 4)):
        tok_step(h, s)
    tok_done(0)
    w_arrive(0)
    blend(0, False)
    forward(0)
    tok_step(1, 3)
    reduce(0)
    tok_step(1, 4)
    tok_done(1)
    forward(1)
    middle(0)
    reduce(1)
    spread(0)
    tok_turn(0)
    middle(1)
    gathered(0)
    turn(0)
    spread(1)
    tok_turn(1)
    w_arrive(1)
    blend(1, False)
    forward(2)
    forward(3)
    reduce(2)
    gathered(1)
    turn(1)
    reduce(3)
    middle(2)
    bend(0)
    spread(2)
    middle(3)
    w_arrive(2)
    blend(2, False)
    forward(4)
    w_arrive(3)
    blend(3, False)
    forward(5)
    spread(3)
    reduce(4)
    forward(6)
    gathered(2)
    turn(2)
    reduce(5)
    middle(4)
    forward(7)
    gathered(3)
    turn(3)
    spread(4)
    reduce(6)
    middle(5)
    bend(1)
    reduce(7)
    spread(5)
    middle(6)
    bend_out(0)
    gathered(4)
    turn(4)
    middle(7)
    hid_copy.start()
    gathered(5)
    turn(5)
    spread(6)
    back(0, 0)
    back_step(0, 0)
    back(0, 1)
    spread(7)
    back_step(0, 1)
    back(0, 2)
    back_step(0, 2)
    gathered(6)
    turn(6)
    back(0, 3)
    gathered(7)
    turn(7)
    back(1, 0)
    back_step(0, 3)
    back_step(1, 0)
    back(1, 1)
    back(0, 4)
    back_step(1, 1)
    back_last(0)
    back(1, 2)
    bend(2)
    back_step(1, 2)
    back(1, 3)
    bend(3)
    back_step(1, 3)
    back(1, 4)
    bend_out(1)
    back_out(0)
    back_last(1)
    bend_out(2)
    bend_out(3)
    back_out(1)
    ig_copy.start()

    hid_copy.wait()
    pltpu.make_async_copy(dw, dw, o_s.at[2]).wait()

    @pl.when(away)
    def _():
        left(tokt, p0_s.at[0], p0_r.at[0, 0], dev_p)
        left(fs.at[0], f_s.at[0], f_r.at[0, 0], dev_p)

    left(tokt, p0_s.at[1], p0_r.at[0, 1], dev_d2)
    left(fs.at[1], f_s.at[1], f_r.at[0, 1], dev_s2)
    left(raw, w_s.at[0], w_r.at[0], dev_y)
    left(ysend, y_s.at[0], y_r.at[0], dev_y)
    left(fbuf.at[pl.ds(0, 3)], x_s.at[0], x_r.at[0, 0], dev_xp)
    for h in range(NH):
        r0, rn = TOKS[h]
        rows = pl.ds(r0, rn)
        left(zs.at[pl.ds(0, 14), rows, :], tz_s.at[h], tz_r.at[h, 0, 0], dev_z[0])
        left(zs.at[pl.ds(0, 14), rows, :], dz_s.at[h], dz_r.at[h, 0, 0], dev_z[0])
        left(dxs.at[:, rows, :], td_s.at[h], td_r.at[h], dev_c)
        left(dxs.at[:, rows, :], dd_s.at[h], dd_r.at[h, 0], dev_c)
    ig_copy.wait()


def hand_on(*refs):
    srcs, dsts, held = refs[0:4], refs[4:8], refs[8:12]
    s_in, s_out = refs[12], refs[13]
    ins = [pltpu.make_async_copy(srcs[i], held[i], s_in.at[i]) for i in range(4)]
    outs = [pltpu.make_async_copy(held[i], dsts[i], s_out.at[i]) for i in range(4)]
    for i in range(4):
        ins[i].start()
    for i in range(4):
        ins[i].wait()
        outs[i].start()
    for i in range(4):
        outs[i].wait()


def per_device(tokens, t_values, *rest):
    a = pl.BlockSpec(memory_space=pl.ANY)
    dma = pltpu.SemaphoreType.DMA
    vm = pltpu.VMEM
    scratch = [
        pltpu.SMEM((8,), F32),
        vm((512, 128), BF),
        vm((128, 512), BF),
        vm((3, 896, 512), BF),
        vm((3, 896, 512), BF),
        vm((448, 512), BF),
        vm((448, 512), BF),
        vm((512, 128), BF),
        vm((4, 1024, 512), BF),
        vm((4, 512, 1024), BF),
        vm((4, 896, 1024), BF),
        vm((4, 896, 512), F32),
        vm((3, 896, 512), BF),
        vm((896, 512), BF),
        vm((2, 896, 512), BF),
        vm((4, 896, 512), BF),
        vm((4, 512, 896), BF),
        vm((896, 512), F32),
        vm((896, 512), BF),
        vm((896, 512), BF),
        vm((16, 512, 128), F32),
        vm((16, 512, 128), BF),
        vm((16, 512, 128), BF),
        vm((16, 512, 128), BF),
        vm((16, 512, 128), BF),
        vm((2, 512, 128), BF),
        vm((2, 512, 128), BF),
        dma((3 + NF,)),
        dma((3,)),
    ]
    for out, into in (((2,), (NH, 2)), ((NH,), (NH, 4, 2)), ((NH,), (NH,)), ((1,), (NF,)), ((1,), (NC, 4)),
                      ((1,), (NF,)), ((NH,), (NH, 5)), ((NH,), (NH, 4, 2)), ((2,), (NH, 2))):
        scratch += [dma(out), dma(into)]
    shapes = (
        jax.ShapeDtypeStruct((448, 512), BF),
        jax.ShapeDtypeStruct((512, 128), BF),
        jax.ShapeDtypeStruct((448, 512), F32),
        jax.ShapeDtypeStruct((448, 512), F32),
    )
    results = pl.pallas_call(
        kernel,
        out_shape=shapes,
        in_specs=[a] * 9,
        out_specs=(a, a, a, a),
        scratch_shapes=scratch,
        compiler_params=pltpu.CompilerParams(
            collective_id=0, has_side_effects=True, vmem_limit_bytes=67_043_328
        ),
    )(tokens, t_values, *(w.T for w in rest))
    hidden, input_grad, gate_grad, up_grad = pl.pallas_call(
        hand_on,
        out_shape=shapes,
        in_specs=[a] * 4,
        out_specs=(a, a, a, a),
        scratch_shapes=[vm(v.shape, v.dtype) for v in shapes] + [dma((4,)), dma((4,))],
    )(*results)
    return hidden.T, input_grad, gate_grad.T, up_grad.T


def solution(mesh):
    return jax.shard_map(
        per_device,
        mesh=mesh,
        in_specs=(P("pt", "tp"), P()) + (P("pt", "tp"),) * 7,
        out_specs=(P("pt", "tp"),) * 4,
        check_vma=False,
    )
```

```python
import jax
import jax.numpy as jnp
from jax import lax
from jax.experimental import pallas as pl
from jax.experimental.pallas import tpu as pltpu
from jax.sharding import PartitionSpec as P

MESH = pl.DeviceIdType.MESH
F32, BF = jnp.float32, jnp.bfloat16

TOKS = ((0, 256), (256, 256))
UNITS = ((0, 256), (256, 256), (512, 256), (768, 128))
CELLS = ((0, 0), (1, 0), (0, 1), (0, 2), (0, 3), (1, 1), (1, 2), (1, 3))
NH, NF, NC = len(TOKS), len(UNITS), len(CELLS)
HOPS = ((4, 3), (3, 4))


def div(a, b):
    return lax.div(a, jnp.int32(b))


def rem(a, b):
    return lax.rem(a, jnp.int32(b))


def mul_of(a, b):
    return pl.multiple_of(a, b)


def kernel(
    tok_in, ts_in, gs, gb, ge, us, ub, ue, hg_in,
    hid_out, ig_out, gg_out, ug_out,
    ts, tok, tokt, raw, rawp, hg, hid, ig, xt, wbuf, fbuf, sbuf, r1, r2, dbuf, dn, dw, ysend, yrecv,
    dxo, dxs, dxr, zs, zr, fs, fr,
    l_s, o_s,
    p0_s, p0_r, tz_s, tz_r, td_s, td_r, w_s, w_r, x_s, x_r, y_s, y_r,
    dd_s, dd_r, dz_s, dz_r, f_s, f_r,
):
    p, t = lax.axis_index("pt"), lax.axis_index("tp")
    x, g = div(p, 2), rem(p, 2)
    yh, z, c = div(t, 16), rem(div(t, 2), 8), rem(t, 2)
    xp, xm, x2 = rem(x + 1, 4), rem(x + 3, 4), rem(x + 2, 4)
    dev_xp, dev_xm = (2 * xp + g, t), (2 * xm + g, t)
    dev_y = (2 * x + (1 - g), t)
    dev_c = (p, yh * 16 + z * 2 + (1 - c))
    dev_z = ((p, yh * 16 + rem(z + 1, 8) * 2 + c), (p, yh * 16 + rem(z + 7, 8) * 2 + c))
    mirror = div(z, 4) != rem(x, 2)
    zq = jnp.where(mirror, 7 - z, z)
    pp, pq = 2 * div(t, 8) + g, div(x, 2) * 16 + zq * 2 + c
    t2 = rem(t + 16, 32)
    dev_p = (pp, pq)
    dev_d2 = (pp, rem(pq + 16, 32))
    dev_s2 = (2 * div(t2, 8) + g, pq)
    away = div(t, 8) != x

    def column(z0):
        return jnp.where(div(z0, 4) != rem(x, 2), 3 - rem(z0, 4), rem(z0, 4))

    mats = ((gs, us), (gb, ub), (ge, ue))

    def units(f):
        c0, cn = UNITS[f]
        return c0, cn, c0 // 2, cn // 2

    tok_load = pltpu.make_async_copy(tok_in, tok, l_s.at[0])
    hg_load = pltpu.make_async_copy(hg_in, hg, l_s.at[1])
    ts_load = pltpu.make_async_copy(ts_in, ts, l_s.at[2])
    tok_load.start()
    for f in range(NF):
        c0, _, u0, un = units(f)
        for m in range(3):
            for k in range(2):
                pltpu.make_async_copy(
                    mats[m][k].at[pl.ds(u0, un), :], raw.at[m, pl.ds(c0 + k * un, un), :], l_s.at[3 + f]).start()
    ts_load.start()
    hg_load.start()

    barrier = pltpu.get_barrier_semaphore()
    for dev in (dev_xp, dev_xm, dev_y, dev_c, dev_z[0], dev_z[1], dev_d2, dev_s2):
        pl.semaphore_signal(barrier, inc=1, device_id=dev, device_id_type=MESH)

    @pl.when(away)
    def _():
        pl.semaphore_signal(barrier, inc=1, device_id=dev_p, device_id_type=MESH)

    tok_load.wait()
    tokt[...] = tok[...].T
    pl.semaphore_wait(barrier, 8 + away.astype(jnp.int32))

    def rc(src, dst, ss, rs, dev):
        return pltpu.make_async_remote_copy(
            src_ref=src, dst_ref=dst, send_sem=ss, recv_sem=rs, device_id=dev, device_id_type=MESH
        )

    def send(src, dst, ss, rs, dev):
        rc(src, dst, ss, rs, dev).start()

    def arrived(dst, ss, rs, dev):
        rc(dst, dst, ss, rs, dev).wait_recv()

    def left(src, ss, rs, dev):
        rc(src, src, ss, rs, dev).wait_send()

    def block(tidx, h):
        r0, rn = TOKS[h]
        return xt.at[tidx[0], pl.ds(mul_of(128 * tidx[1], 128), 128), pl.ds(r0, rn)]

    def tblock(z0, piece, cc, h):
        return block((rem(yh + piece, 2) * 2 + div(z0, 4), column(z0) * 2 + cc), h)

    there = (x, rem(t, 8))

    def tok_scatter(h):
        r0, rn = TOKS[h]
        mine = tokt.at[:, pl.ds(r0, rn)]

        @pl.when(away)
        def _():
            send(mine, block(there, h), p0_s.at[0], p0_r.at[h, 0], dev_p)

        send(mine, block(there, h), p0_s.at[1], p0_r.at[h, 1], dev_d2)

        @pl.when(jnp.logical_not(away))
        def _():
            block(there, h)[...] = tokt[:, pl.ds(r0, rn)]

    def tok_arrive(h, piece):
        b = tblock(z, piece, c, h)
        if piece == 0:
            @pl.when(away)
            def _():
                arrived(b, p0_s.at[0], p0_r.at[h, 0], dev_p)
        else:
            arrived(b, p0_s.at[1], p0_r.at[h, 1], dev_d2)

    def z_at(direction, s):
        return rem(z + 8 - s, 8) if direction == 0 else rem(z + s, 8)

    def ring_wait(h, s, piece):
        r0, rn = TOKS[h]
        n = sum(s < HOPS[d][piece] for d in (0, 1))
        arrived(zr.at[pl.ds(0, n), pl.ds(0, rn), :], tz_s.at[h], tz_r.at[h, s, piece], dev_z[0])

    def tok_step(h, s):
        for piece in (0, 1):
            if s == 0:
                tok_arrive(h, piece)
            elif s <= max(HOPS[0][piece], HOPS[1][piece]):
                ring_wait(h, s - 1, piece)
            for direction in (0, 1):
                if s < HOPS[direction][piece]:
                    b = tblock(z_at(direction, s), piece, c, h)
                    send(b, b, tz_s.at[h], tz_r.at[h, s, piece], dev_z[direction])
            for direction in (0, 1):
                if s <= HOPS[direction][piece] and (s > 0 or direction == 0):
                    b = tblock(z_at(direction, s), piece, c, h)
                    send(b, b, td_s.at[h], td_r.at[h], dev_c)

    def tok_done(h):
        r0, rn = TOKS[h]
        arrived(xt.at[:, pl.ds(0, 512), pl.ds(r0, rn)], td_s.at[h], td_r.at[h], dev_c)

    def w_here(f):
        c0, cn = UNITS[f]
        b = raw.at[:, pl.ds(c0, cn), :]
        pltpu.make_async_copy(b, b, l_s.at[3 + f]).wait()

    def w_send(f):
        c0, cn = UNITS[f]
        b = raw.at[:, pl.ds(c0, cn), :]
        send(b, rawp.at[:, pl.ds(c0, cn), :], w_s.at[0], w_r.at[f], dev_y)

    def w_arrive(f):
        c0, cn = UNITS[f]
        arrived(rawp.at[:, pl.ds(c0, cn), :], w_s.at[0], w_r.at[f], dev_y)

    ts_load.wait()
    tv = [ts[2 * j + g] for j in range(4)]
    coef = [((1.0 - v) * (1.0 - v), 2.0 * v * (1.0 - v), v * v) for v in tv]

    def blend(f, own):
        c0, cn = UNITS[f]
        src, side = (raw, g) if own else (rawp, 1 - g)
        lanes = pl.ds(mul_of(side * 512, 512), 512)

        def one(i, _):
            r = pl.ds(mul_of(c0 + i * 16, 16), 16)
            v = [src[m, r, :].astype(F32) for m in range(3)]
            for j in range(4):
                b0, b1, b2 = coef[j]
                wbuf[j, r, lanes] = (b0 * v[0] + b1 * v[1] + b2 * v[2]).astype(BF)
            return 0

        lax.fori_loop(0, cn // 16, one, 0)

    def cell(i):
        h, f = CELLS[i]
        return TOKS[h] + UNITS[f] + (f,)

    def at(ref, i, half=None):
        r0, rn, c0, cn, _ = cell(i)
        if half is not None:
            c0, cn = c0 + half * (cn // 2), cn // 2
        return ref.at[pl.ds(c0, cn), pl.ds(r0, rn)]

    def forward(i):
        r0, rn, c0, cn, _ = cell(i)

        def one(k, _):
            for q in (2 * k, 2 * k + 1):
                jr = rem(x + q, 4)
                fbuf[q, c0:c0 + cn, r0:r0 + rn] = jnp.dot(
                    wbuf[jr, c0:c0 + cn, :], xt[jr, :, r0:r0 + rn], preferred_element_type=F32)
            return 0

        lax.fori_loop(0, 2, one, 0)
        sbuf[0, c0:c0 + cn, r0:r0 + rn] = fbuf[2, c0:c0 + cn, r0:r0 + rn].astype(BF)
        send(at(sbuf.at[0], i, 0), at(r1, i, 0), x_s.at[0], x_r.at[i, 0], dev_xp)
        send(at(sbuf.at[0], i, 1), at(r1, i, 1), x_s.at[0], x_r.at[i, 0], dev_xm)

    def reduce(i):
        r0, rn, c0, cn, _ = cell(i)
        n = cn // 2
        a, b, cs = slice(c0, c0 + n), slice(c0 + n, c0 + cn), slice(r0, r0 + rn)
        arrived(at(r1, i), x_s.at[0], x_r.at[i, 0], dev_xm)
        sbuf[1, a, cs] = (fbuf[1, a, cs] + r1[a, cs].astype(F32)).astype(BF)
        sbuf[1, b, cs] = fbuf[1, b, cs].astype(BF)
        send(at(sbuf.at[1], i), at(r2.at[0], i), x_s.at[0], x_r.at[i, 1], dev_xp)
        sbuf[2, a, cs] = fbuf[3, a, cs].astype(BF)
        sbuf[2, b, cs] = (fbuf[3, b, cs] + r1[b, cs].astype(F32)).astype(BF)
        send(at(sbuf.at[2], i), at(r2.at[1], i), x_s.at[0], x_r.at[i, 1], dev_xm)

    def two(i):
        r0, rn, c0, cn, _ = cell(i)
        return r2.at[:, pl.ds(c0, cn), pl.ds(r0, rn)]

    def middle(i):
        r0, rn, c0, cn, f = cell(i)
        arrived(two(i), x_s.at[0], x_r.at[i, 1], dev_xm)
        cs = slice(r0, r0 + rn)

        def total(r):
            return fbuf[0, r, cs] + r2[0, r, cs].astype(F32) + r2[1, r, cs].astype(F32)

        def one(k, _):
            rg = pl.ds(mul_of(c0 + k * 16, 16), 16)
            ru = pl.ds(mul_of(c0 + cn // 2 + k * 16, 16), 16)
            rh = pl.ds(mul_of(c0 // 2 + k * 16, 16), 16)
            gate, up = total(rg), total(ru)
            cot = hg[rh, cs].astype(F32)
            sig = jax.nn.sigmoid(gate)
            act = gate * sig
            hid[rh, cs] = (act * up).astype(BF)
            dbuf[x, rg, cs] = (cot * up * sig * (1.0 + gate * (1.0 - sig))).astype(BF)
            dbuf[x, ru, cs] = (cot * act).astype(BF)
            return 0

        lax.fori_loop(0, cn // 32, one, 0)
        send(at(dbuf.at[x], i), at(dbuf.at[x], i), x_s.at[0], x_r.at[i, 2], dev_xp)
        send(at(dbuf.at[x], i), at(dbuf.at[x], i), x_s.at[0], x_r.at[i, 2], dev_xm)

    def spread(i):
        arrived(two(i), x_s.at[0], x_r.at[i, 2], dev_xm)
        b = at(dbuf.at[xm], i, 0)
        send(b, b, x_s.at[0], x_r.at[i, 3], dev_xp)
        b = at(dbuf.at[xp], i, 1)
        send(b, b, x_s.at[0], x_r.at[i, 3], dev_xm)

    def gathered(i):
        arrived(at(r1, i), x_s.at[0], x_r.at[i, 3], dev_xm)

    def turn(i):
        r0, rn, c0, cn, _ = cell(i)

        def one(j, _):
            dn[j, r0:r0 + rn, c0:c0 + cn] = dbuf[j, c0:c0 + cn, r0:r0 + rn].T
            return 0

        lax.fori_loop(0, 4, one, 0)

    def bend(f):
        c0, cn = UNITS[f]

        def part(lanes):
            acc = None
            for j in range(4):
                d = coef[j][1] * lax.dot_general(dbuf[j, c0:c0 + cn, :], xt[j, lanes, :], (((1,), (1,)), ((), ())),
                                                 preferred_element_type=F32)
                acc = d if acc is None else acc + d
            return acc

        def one(k, _):
            q = rem(k, 2)
            mine = part(pl.ds(mul_of(rem(1 - g + div(k, 2), 2) * 512 + q * 256, 256), 256))
            r = pl.ds(mul_of(q * 256, 256), 256)

            @pl.when(k < 2)
            def _():
                ysend[c0:c0 + cn, r] = mine.astype(BF)

            @pl.when(k >= 2)
            def _():
                dw[c0:c0 + cn, r] = mine
            return 0

        lax.fori_loop(0, 4, one, 0)
        send(ysend.at[pl.ds(c0, cn), :], yrecv.at[pl.ds(c0, cn), :], y_s.at[0], y_r.at[f], dev_y)

    def dw_out(f, k):
        c0, _, u0, un = units(f)
        return pltpu.make_async_copy(
            dw.at[pl.ds(c0 + k * un, un), :], (gg_out, ug_out)[k].at[pl.ds(u0, un), :], o_s.at[2])

    hid_copy = pltpu.make_async_copy(hid, hid_out, o_s.at[0])
    ig_copy = pltpu.make_async_copy(ig, ig_out, o_s.at[1])

    def bend_out(f):
        c0, cn = UNITS[f]
        arrived(yrecv.at[pl.ds(c0, cn), :], y_s.at[0], y_r.at[f], dev_y)

        def one(k, _):
            r = pl.ds(mul_of(c0 + k * 32, 32), 32)
            dw[r, :] = dw[r, :] + yrecv[r, :].astype(F32)
            return 0

        lax.fori_loop(0, cn // 32, one, 0)
        dw_out(f, 0).start()
        dw_out(f, 1).start()

    def back(h, part):
        r0, rn = TOKS[h]
        rows = pl.ds(r0, rn)

        def one(piece, _):
            for k in ((4,), (3, 5), (2, 6), (1, 7), (0,))[part]:
                zd, yd = rem(z + k, 8), rem(yh + piece, 2)
                jr = yd * 2 + div(zd, 4)
                v = jnp.dot(dn[jr, r0:r0 + rn, :], wbuf[jr, :, pl.ds(mul_of(256 * column(zd), 256), 256)],
                            preferred_element_type=F32)
                s = k * 2 + piece
                dxo[s, r0:r0 + rn, :] = jnp.where(c == 0, v[:, 0:128], v[:, 128:256])
                dxs[s, r0:r0 + rn, :] = jnp.where(c == 0, v[:, 128:256], v[:, 0:128]).astype(BF)
                send(dxs.at[s, rows, :], dxr.at[s, rows, :], dd_s.at[h], dd_r.at[h, part], dev_c)
            return 0

        lax.fori_loop(0, 2, one, 0)

    def core_sum(h, piece, k):
        r0, rn = TOKS[h]
        s = k * 2 + piece
        return dxo[s, r0:r0 + rn, :] + dxr[s, r0:r0 + rn, :].astype(F32)

    def core_wait(h, part):
        r0, rn = TOKS[h]
        n = 2 if part in (0, 4) else 4
        arrived(dxr.at[pl.ds(0, n), pl.ds(r0, rn), :], dd_s.at[h], dd_r.at[h, part], dev_c)

    def zslot(direction, piece, s):
        return (direction * 2 + piece) * 4 + s

    def back_wait(h, s, piece):
        r0, rn = TOKS[h]
        n = sum(s >= 4 - HOPS[d][piece] for d in (0, 1))
        arrived(zr.at[pl.ds(0, n), pl.ds(r0, rn), :], dz_s.at[h], dz_r.at[h, s, piece], dev_z[0])

    def back_step(h, s):
        r0, rn = TOKS[h]
        core_wait(h, s)
        for piece in (0, 1):
            if s > 4 - max(HOPS[0][piece], HOPS[1][piece]):
                back_wait(h, s - 1, piece)
            for direction in (0, 1):
                first = 4 - HOPS[direction][piece]
                if s < first:
                    continue
                k = 4 - s if direction == 0 else 4 + s
                v = core_sum(h, piece, k)
                if s > first:
                    v = v + zr[zslot(direction, piece, s - 1), r0:r0 + rn, :].astype(F32)
                i = zslot(direction, piece, s)
                zs[i, r0:r0 + rn, :] = v.astype(BF)
                send(zs.at[i, pl.ds(r0, rn), :], zr.at[i, pl.ds(r0, rn), :], dz_s.at[h], dz_r.at[h, s, piece],
                     dev_z[direction])

    def back_last(h):
        r0, rn = TOKS[h]
        rows = pl.ds(r0, rn)
        core_wait(h, 4)
        for piece in (0, 1):
            back_wait(h, 3, piece)
            v = core_sum(h, piece, 0)
            for direction in (0, 1):
                v = v + zr[zslot(direction, piece, 3), r0:r0 + rn, :].astype(F32)
            fs[piece, r0:r0 + rn, :] = v.astype(BF)
            if piece == 0:
                @pl.when(away)
                def _():
                    send(fs.at[0, rows, :], fr.at[0, rows, :], f_s.at[0], f_r.at[h, 0], dev_p)

                @pl.when(jnp.logical_not(away))
                def _():
                    fr[0, r0:r0 + rn, :] = fs[0, r0:r0 + rn, :]
            else:
                send(fs.at[1, rows, :], fr.at[1, rows, :], f_s.at[1], f_r.at[h, 1], dev_s2)

    def back_out(h):
        r0, rn = TOKS[h]
        rows = pl.ds(r0, rn)

        @pl.when(away)
        def _():
            arrived(fr.at[0, rows, :], f_s.at[0], f_r.at[h, 0], dev_p)

        arrived(fr.at[1, rows, :], f_s.at[1], f_r.at[h, 1], dev_d2)
        ig[r0:r0 + rn, :] = (fr[0, r0:r0 + rn, :].astype(F32) + fr[1, r0:r0 + rn, :].astype(F32)).astype(BF)

    tok_scatter(0)
    tok_scatter(1)
    w_here(0)
    w_send(0)
    w_here(1)
    w_send(1)
    w_here(2)
    w_send(2)
    w_here(3)
    w_send(3)
    blend(0, True)
    blend(1, True)
    blend(2, True)
    blend(3, True)
    tok_step(0, 0)
    tok_step(1, 0)
    tok_step(0, 1)
    tok_step(0, 2)
    w_arrive(0)
    tok_step(1, 1)
    tok_step(0, 3)
    blend(0, False)
    tok_step(1, 2)
    tok_step(0, 4)
    tok_done(0)
    forward(0)
    tok_step(1, 3)
    reduce(0)
    w_arrive(1)
    tok_step(1, 4)
    blend(1, False)
    forward(2)
    tok_done(1)
    forward(5)
    forward(1)
    hg_load.wait()
    middle(0)
    reduce(2)
    reduce(5)
    reduce(1)
    spread(0)
    w_arrive(2)
    blend(2, False)
    forward(3)
    forward(6)
    middle(2)
    reduce(3)
    w_arrive(3)
    blend(3, False)
    forward(4)
    forward(7)
    reduce(6)
    reduce(4)
    gathered(0)
    turn(0)
    reduce(7)
    middle(3)
    middle(4)
    middle(7)
    spread(2)
    spread(3)
    spread(4)
    middle(5)
    middle(6)
    gathered(2)
    turn(2)
    middle(1)
    hid_copy.start()
    gathered(3)
    turn(3)
    gathered(4)
    turn(4)
    spread(7)
    back(0, 0)
    back(0, 1)
    back_step(0, 0)
    back(0, 2)
    back(0, 4)
    spread(5)
    back_step(0, 1)
    spread(6)
    spread(1)
    back(0, 3)
    gathered(5)
    turn(5)
    gathered(7)
    turn(7)
    back_step(0, 2)
    gathered(6)
    turn(6)
    gathered(1)
    turn(1)
    back(1, 0)
    back_step(1, 0)
    bend(2)
    back(1, 1)
    back_step(0, 3)
    back_step(1, 1)
    bend(0)
    back(1, 2)
    back_last(0)
    back_step(1, 2)
    bend(1)
    back(1, 3)
    back_step(1, 3)
    bend(3)
    back(1, 4)
    back_last(1)
    bend_out(2)
    bend_out(0)
    back_out(0)
    bend_out(1)
    bend_out(3)
    back_out(1)
    ig_copy.start()

    hid_copy.wait()
    pltpu.make_async_copy(dw, dw, o_s.at[2]).wait()

    @pl.when(away)
    def _():
        left(tokt, p0_s.at[0], p0_r.at[0, 0], dev_p)
        left(fs.at[0], f_s.at[0], f_r.at[0, 0], dev_p)

    left(tokt, p0_s.at[1], p0_r.at[0, 1], dev_d2)
    left(fs.at[1], f_s.at[1], f_r.at[0, 1], dev_s2)
    left(raw, w_s.at[0], w_r.at[0], dev_y)
    left(ysend, y_s.at[0], y_r.at[0], dev_y)
    left(fbuf.at[pl.ds(0, 3)], x_s.at[0], x_r.at[0, 0], dev_xp)
    for h in range(NH):
        r0, rn = TOKS[h]
        rows = pl.ds(r0, rn)
        left(zs.at[pl.ds(0, 14), rows, :], tz_s.at[h], tz_r.at[h, 0, 0], dev_z[0])
        left(zs.at[pl.ds(0, 14), rows, :], dz_s.at[h], dz_r.at[h, 0, 0], dev_z[0])
        left(dxs.at[:, rows, :], td_s.at[h], td_r.at[h], dev_c)
        left(dxs.at[:, rows, :], dd_s.at[h], dd_r.at[h, 0], dev_c)
    ig_copy.wait()


def hand_on(*refs):
    srcs, dsts, held = refs[0:4], refs[4:8], refs[8:12]
    s_in, s_out = refs[12], refs[13]
    ins = [pltpu.make_async_copy(srcs[i], held[i], s_in.at[i]) for i in range(4)]
    outs = [pltpu.make_async_copy(held[i], dsts[i], s_out.at[i]) for i in range(4)]
    for i in range(4):
        ins[i].start()
    for i in range(4):
        ins[i].wait()
        outs[i].start()
    for i in range(4):
        outs[i].wait()


def per_device(tokens, t_values, *rest):
    a = pl.BlockSpec(memory_space=pl.ANY)
    dma = pltpu.SemaphoreType.DMA
    vm = pltpu.VMEM
    scratch = [
        pltpu.SMEM((8,), F32),
        vm((512, 128), BF),
        vm((128, 512), BF),
        vm((3, 896, 512), BF),
        vm((3, 896, 512), BF),
        vm((448, 512), BF),
        vm((448, 512), BF),
        vm((512, 128), BF),
        vm((4, 1024, 512), BF),
        vm((4, 896, 1024), BF),
        vm((4, 896, 512), F32),
        vm((3, 896, 512), BF),
        vm((896, 512), BF),
        vm((2, 896, 512), BF),
        vm((4, 896, 512), BF),
        vm((4, 512, 896), BF),
        vm((896, 512), F32),
        vm((896, 512), BF),
        vm((896, 512), BF),
        vm((16, 512, 128), F32),
        vm((16, 512, 128), BF),
        vm((16, 512, 128), BF),
        vm((16, 512, 128), BF),
        vm((16, 512, 128), BF),
        vm((2, 512, 128), BF),
        vm((2, 512, 128), BF),
        dma((3 + NF,)),
        dma((3,)),
    ]
    for out, into in (((2,), (NH, 2)), ((NH,), (NH, 4, 2)), ((NH,), (NH,)), ((1,), (NF,)), ((1,), (NC, 4)),
                      ((1,), (NF,)), ((NH,), (NH, 5)), ((NH,), (NH, 4, 2)), ((2,), (NH, 2))):
        scratch += [dma(out), dma(into)]
    shapes = (
        jax.ShapeDtypeStruct((448, 512), BF),
        jax.ShapeDtypeStruct((512, 128), BF),
        jax.ShapeDtypeStruct((448, 512), F32),
        jax.ShapeDtypeStruct((448, 512), F32),
    )
    results = pl.pallas_call(
        kernel,
        out_shape=shapes,
        in_specs=[a] * 9,
        out_specs=(a, a, a, a),
        scratch_shapes=scratch,
        compiler_params=pltpu.CompilerParams(
            collective_id=0, has_side_effects=True, vmem_limit_bytes=67_043_328
        ),
    )(tokens, t_values, *(w.T for w in rest))
    hidden, input_grad, gate_grad, up_grad = pl.pallas_call(
        hand_on,
        out_shape=shapes,
        in_specs=[a] * 4,
        out_specs=(a, a, a, a),
        scratch_shapes=[vm(v.shape, v.dtype) for v in shapes] + [dma((4,)), dma((4,))],
    )(*results)
    return hidden.T, input_grad, gate_grad.T, up_grad.T


def solution(mesh):
    return jax.shard_map(
        per_device,
        mesh=mesh,
        in_specs=(P("pt", "tp"), P()) + (P("pt", "tp"),) * 7,
        out_specs=(P("pt", "tp"),) * 4,
        check_vma=False,
    )
```

```python
import jax
import jax.numpy as jnp
from jax import lax
from jax.experimental import pallas as pl
from jax.experimental.pallas import tpu as pltpu
from jax.sharding import PartitionSpec as P

MESH = pl.DeviceIdType.MESH
F32, BF = jnp.float32, jnp.bfloat16

TOKS = ((0, 256), (256, 256))
UNITS = ((0, 256), (256, 256), (512, 256), (768, 128))
CELLS = ((0, 0), (1, 0), (0, 1), (0, 2), (0, 3), (1, 1), (1, 2), (1, 3))
NH, NF, NC = len(TOKS), len(UNITS), len(CELLS)
HOPS = ((4, 3), (3, 4))


def div(a, b):
    return lax.div(a, jnp.int32(b))


def rem(a, b):
    return lax.rem(a, jnp.int32(b))


def mul_of(a, b):
    return pl.multiple_of(a, b)


def kernel(
    tok_in, ts_in, gs, gb, ge, us, ub, ue, hg_in,
    hid_out, ig_out, gg_out, ug_out,
    ts, tok, tokt, raw, rawp, hg, hid, ig, xt, wbuf, fbuf, sbuf, r1, r2, dbuf, dn, dw, ysend, yrecv,
    dxo, dxs, dxr, zs, zr, fs, fr,
    l_s, o_s,
    p0_s, p0_r, tz_s, tz_r, td_s, td_r, w_s, w_r, x_s, x_r, y_s, y_r,
    dd_s, dd_r, dz_s, dz_r, f_s, f_r,
):
    p, t = lax.axis_index("pt"), lax.axis_index("tp")
    x, g = div(p, 2), rem(p, 2)
    yh, z, c = div(t, 16), rem(div(t, 2), 8), rem(t, 2)
    xp, xm, x2 = rem(x + 1, 4), rem(x + 3, 4), rem(x + 2, 4)
    dev_xp, dev_xm = (2 * xp + g, t), (2 * xm + g, t)
    dev_y = (2 * x + (1 - g), t)
    dev_c = (p, yh * 16 + z * 2 + (1 - c))
    dev_z = ((p, yh * 16 + rem(z + 1, 8) * 2 + c), (p, yh * 16 + rem(z + 7, 8) * 2 + c))
    mirror = div(z, 4) != rem(x, 2)
    zq = jnp.where(mirror, 7 - z, z)
    pp, pq = 2 * div(t, 8) + g, div(x, 2) * 16 + zq * 2 + c
    t2 = rem(t + 16, 32)
    dev_p = (pp, pq)
    dev_d2 = (pp, rem(pq + 16, 32))
    dev_s2 = (2 * div(t2, 8) + g, pq)
    away = div(t, 8) != x

    def column(z0):
        return jnp.where(div(z0, 4) != rem(x, 2), 3 - rem(z0, 4), rem(z0, 4))

    mats = ((gs, us), (gb, ub), (ge, ue))

    def units(f):
        c0, cn = UNITS[f]
        return c0, cn, c0 // 2, cn // 2

    tok_load = pltpu.make_async_copy(tok_in, tok, l_s.at[0])
    hg_load = pltpu.make_async_copy(hg_in, hg, l_s.at[1])
    ts_load = pltpu.make_async_copy(ts_in, ts, l_s.at[2])
    tok_load.start()
    for f in range(NF):
        c0, _, u0, un = units(f)
        for m in range(3):
            for k in range(2):
                pltpu.make_async_copy(
                    mats[m][k].at[pl.ds(u0, un), :], raw.at[m, pl.ds(c0 + k * un, un), :], l_s.at[3 + f]).start()
    ts_load.start()
    hg_load.start()

    barrier = pltpu.get_barrier_semaphore()
    for dev in (dev_xp, dev_xm, dev_y, dev_c, dev_z[0], dev_z[1], dev_d2, dev_s2):
        pl.semaphore_signal(barrier, inc=1, device_id=dev, device_id_type=MESH)

    @pl.when(away)
    def _():
        pl.semaphore_signal(barrier, inc=1, device_id=dev_p, device_id_type=MESH)

    tok_load.wait()
    tokt[...] = tok[...].T
    pl.semaphore_wait(barrier, 8 + away.astype(jnp.int32))

    def rc(src, dst, ss, rs, dev):
        return pltpu.make_async_remote_copy(
            src_ref=src, dst_ref=dst, send_sem=ss, recv_sem=rs, device_id=dev, device_id_type=MESH
        )

    def send(src, dst, ss, rs, dev):
        rc(src, dst, ss, rs, dev).start()

    def arrived(dst, ss, rs, dev):
        rc(dst, dst, ss, rs, dev).wait_recv()

    def left(src, ss, rs, dev):
        rc(src, src, ss, rs, dev).wait_send()

    def block(tidx, h):
        r0, rn = TOKS[h]
        return xt.at[tidx[0], pl.ds(mul_of(128 * tidx[1], 128), 128), pl.ds(r0, rn)]

    def tblock(z0, piece, cc, h):
        return block((rem(yh + piece, 2) * 2 + div(z0, 4), column(z0) * 2 + cc), h)

    there = (x, rem(t, 8))

    def tok_scatter(h):
        r0, rn = TOKS[h]
        mine = tokt.at[:, pl.ds(r0, rn)]

        @pl.when(away)
        def _():
            send(mine, block(there, h), p0_s.at[0], p0_r.at[h, 0], dev_p)

        send(mine, block(there, h), p0_s.at[1], p0_r.at[h, 1], dev_d2)

        @pl.when(jnp.logical_not(away))
        def _():
            block(there, h)[...] = tokt[:, pl.ds(r0, rn)]

    def tok_arrive(h, piece):
        b = tblock(z, piece, c, h)
        if piece == 0:
            @pl.when(away)
            def _():
                arrived(b, p0_s.at[0], p0_r.at[h, 0], dev_p)
        else:
            arrived(b, p0_s.at[1], p0_r.at[h, 1], dev_d2)

    def z_at(direction, s):
        return rem(z + 8 - s, 8) if direction == 0 else rem(z + s, 8)

    def ring_wait(h, s, piece):
        r0, rn = TOKS[h]
        n = sum(s < HOPS[d][piece] for d in (0, 1))
        arrived(zr.at[pl.ds(0, n), pl.ds(0, rn), :], tz_s.at[h], tz_r.at[h, s, piece], dev_z[0])

    def tok_step(h, s):
        for piece in (0, 1):
            if s == 0:
                tok_arrive(h, piece)
            elif s <= max(HOPS[0][piece], HOPS[1][piece]):
                ring_wait(h, s - 1, piece)
            for direction in (0, 1):
                if s < HOPS[direction][piece]:
                    b = tblock(z_at(direction, s), piece, c, h)
                    send(b, b, tz_s.at[h], tz_r.at[h, s, piece], dev_z[direction])
            for direction in (0, 1):
                if s <= HOPS[direction][piece] and (s > 0 or direction == 0):
                    b = tblock(z_at(direction, s), piece, c, h)
                    send(b, b, td_s.at[h], td_r.at[h], dev_c)

    def tok_done(h):
        r0, rn = TOKS[h]
        arrived(xt.at[:, pl.ds(0, 512), pl.ds(r0, rn)], td_s.at[h], td_r.at[h], dev_c)

    def w_here(f):
        c0, cn = UNITS[f]
        b = raw.at[:, pl.ds(c0, cn), :]
        pltpu.make_async_copy(b, b, l_s.at[3 + f]).wait()

    def w_send(f):
        c0, cn = UNITS[f]
        b = raw.at[:, pl.ds(c0, cn), :]
        send(b, rawp.at[:, pl.ds(c0, cn), :], w_s.at[0], w_r.at[f], dev_y)

    def w_arrive(f):
        c0, cn = UNITS[f]
        arrived(rawp.at[:, pl.ds(c0, cn), :], w_s.at[0], w_r.at[f], dev_y)

    ts_load.wait()
    tv = [ts[2 * j + g] for j in range(4)]
    coef = [((1.0 - v) * (1.0 - v), 2.0 * v * (1.0 - v), v * v) for v in tv]

    def blend(f, own):
        c0, cn = UNITS[f]
        src, side = (raw, g) if own else (rawp, 1 - g)
        lanes = pl.ds(mul_of(side * 512, 512), 512)

        def one(i, _):
            r = pl.ds(mul_of(c0 + i * 16, 16), 16)
            v = [src[m, r, :].astype(F32) for m in range(3)]
            for j in range(4):
                b0, b1, b2 = coef[j]
                wbuf[j, r, lanes] = (b0 * v[0] + b1 * v[1] + b2 * v[2]).astype(BF)
            return 0

        lax.fori_loop(0, cn // 16, one, 0)

    def cell(i):
        h, f = CELLS[i]
        return TOKS[h] + UNITS[f] + (f,)

    def at(ref, i, half=None):
        r0, rn, c0, cn, _ = cell(i)
        if half is not None:
            c0, cn = c0 + half * (cn // 2), cn // 2
        return ref.at[pl.ds(c0, cn), pl.ds(r0, rn)]

    def forward(i):
        r0, rn, c0, cn, _ = cell(i)

        def one(k, _):
            for q in (2 * k, 2 * k + 1):
                jr = rem(x + q, 4)
                fbuf[q, c0:c0 + cn, r0:r0 + rn] = jnp.dot(
                    wbuf[jr, c0:c0 + cn, :], xt[jr, :, r0:r0 + rn], preferred_element_type=F32)
            return 0

        lax.fori_loop(0, 2, one, 0)
        sbuf[0, c0:c0 + cn, r0:r0 + rn] = fbuf[2, c0:c0 + cn, r0:r0 + rn].astype(BF)
        send(at(sbuf.at[0], i, 0), at(r1, i, 0), x_s.at[0], x_r.at[i, 0], dev_xp)
        send(at(sbuf.at[0], i, 1), at(r1, i, 1), x_s.at[0], x_r.at[i, 0], dev_xm)

    def reduce(i):
        r0, rn, c0, cn, _ = cell(i)
        n = cn // 2
        a, b, cs = slice(c0, c0 + n), slice(c0 + n, c0 + cn), slice(r0, r0 + rn)
        arrived(at(r1, i), x_s.at[0], x_r.at[i, 0], dev_xm)
        sbuf[1, a, cs] = (fbuf[1, a, cs] + r1[a, cs].astype(F32)).astype(BF)
        sbuf[1, b, cs] = fbuf[1, b, cs].astype(BF)
        send(at(sbuf.at[1], i), at(r2.at[0], i), x_s.at[0], x_r.at[i, 1], dev_xp)
        sbuf[2, a, cs] = fbuf[3, a, cs].astype(BF)
        sbuf[2, b, cs] = (fbuf[3, b, cs] + r1[b, cs].astype(F32)).astype(BF)
        send(at(sbuf.at[2], i), at(r2.at[1], i), x_s.at[0], x_r.at[i, 1], dev_xm)

    def two(i):
        r0, rn, c0, cn, _ = cell(i)
        return r2.at[:, pl.ds(c0, cn), pl.ds(r0, rn)]

    def middle(i):
        r0, rn, c0, cn, f = cell(i)
        arrived(two(i), x_s.at[0], x_r.at[i, 1], dev_xm)
        cs = slice(r0, r0 + rn)

        def total(r):
            return fbuf[0, r, cs] + r2[0, r, cs].astype(F32) + r2[1, r, cs].astype(F32)

        def one(k, _):
            rg = pl.ds(mul_of(c0 + k * 16, 16), 16)
            ru = pl.ds(mul_of(c0 + cn // 2 + k * 16, 16), 16)
            rh = pl.ds(mul_of(c0 // 2 + k * 16, 16), 16)
            gate, up = total(rg), total(ru)
            cot = hg[rh, cs].astype(F32)
            sig = jax.nn.sigmoid(gate)
            act = gate * sig
            hid[rh, cs] = (act * up).astype(BF)
            dbuf[x, rg, cs] = (cot * up * sig * (1.0 + gate * (1.0 - sig))).astype(BF)
            dbuf[x, ru, cs] = (cot * act).astype(BF)
            return 0

        lax.fori_loop(0, cn // 32, one, 0)
        send(at(dbuf.at[x], i), at(dbuf.at[x], i), x_s.at[0], x_r.at[i, 2], dev_xp)
        send(at(dbuf.at[x], i), at(dbuf.at[x], i), x_s.at[0], x_r.at[i, 2], dev_xm)

    def spread(i):
        arrived(two(i), x_s.at[0], x_r.at[i, 2], dev_xm)
        b = at(dbuf.at[xm], i, 0)
        send(b, b, x_s.at[0], x_r.at[i, 3], dev_xp)
        b = at(dbuf.at[xp], i, 1)
        send(b, b, x_s.at[0], x_r.at[i, 3], dev_xm)

    def gathered(i):
        arrived(at(r1, i), x_s.at[0], x_r.at[i, 3], dev_xm)

    def turn(i):
        r0, rn, c0, cn, _ = cell(i)

        def one(j, _):
            dn[j, r0:r0 + rn, c0:c0 + cn] = dbuf[j, c0:c0 + cn, r0:r0 + rn].T
            return 0

        lax.fori_loop(0, 4, one, 0)

    def bend(f):
        c0, cn = UNITS[f]

        def part(lanes):
            acc = None
            for j in range(4):
                d = coef[j][1] * lax.dot_general(dbuf[j, c0:c0 + cn, :], xt[j, lanes, :], (((1,), (1,)), ((), ())),
                                                 preferred_element_type=F32)
                acc = d if acc is None else acc + d
            return acc

        def one(k, _):
            q = rem(k, 2)
            mine = part(pl.ds(mul_of(rem(1 - g + div(k, 2), 2) * 512 + q * 256, 256), 256))
            r = pl.ds(mul_of(q * 256, 256), 256)

            @pl.when(k < 2)
            def _():
                ysend[c0:c0 + cn, r] = mine.astype(BF)

            @pl.when(k >= 2)
            def _():
                dw[c0:c0 + cn, r] = mine
            return 0

        lax.fori_loop(0, 4, one, 0)
        send(ysend.at[pl.ds(c0, cn), :], yrecv.at[pl.ds(c0, cn), :], y_s.at[0], y_r.at[f], dev_y)

    def dw_out(f, k):
        c0, _, u0, un = units(f)
        return pltpu.make_async_copy(
            dw.at[pl.ds(c0 + k * un, un), :], (gg_out, ug_out)[k].at[pl.ds(u0, un), :], o_s.at[2])

    hid_copy = pltpu.make_async_copy(hid, hid_out, o_s.at[0])
    ig_copy = pltpu.make_async_copy(ig, ig_out, o_s.at[1])

    def bend_out(f):
        c0, cn = UNITS[f]
        arrived(yrecv.at[pl.ds(c0, cn), :], y_s.at[0], y_r.at[f], dev_y)

        def one(k, _):
            r = pl.ds(mul_of(c0 + k * 32, 32), 32)
            dw[r, :] = dw[r, :] + yrecv[r, :].astype(F32)
            return 0

        lax.fori_loop(0, cn // 32, one, 0)
        dw_out(f, 0).start()
        dw_out(f, 1).start()

    def back(h, part):
        r0, rn = TOKS[h]
        rows = pl.ds(r0, rn)

        def one(piece, _):
            for k in ((4,), (3, 5), (2, 6), (1, 7), (0,))[part]:
                zd, yd = rem(z + k, 8), rem(yh + piece, 2)
                jr = yd * 2 + div(zd, 4)
                v = jnp.dot(dn[jr, r0:r0 + rn, :], wbuf[jr, :, pl.ds(mul_of(256 * column(zd), 256), 256)],
                            preferred_element_type=F32)
                s = k * 2 + piece
                dxo[s, r0:r0 + rn, :] = jnp.where(c == 0, v[:, 0:128], v[:, 128:256])
                dxs[s, r0:r0 + rn, :] = jnp.where(c == 0, v[:, 128:256], v[:, 0:128]).astype(BF)
                send(dxs.at[s, rows, :], dxr.at[s, rows, :], dd_s.at[h], dd_r.at[h, part], dev_c)
            return 0

        lax.fori_loop(0, 2, one, 0)

    def core_sum(h, piece, k):
        r0, rn = TOKS[h]
        s = k * 2 + piece
        return dxo[s, r0:r0 + rn, :] + dxr[s, r0:r0 + rn, :].astype(F32)

    def core_wait(h, part):
        r0, rn = TOKS[h]
        n = 2 if part in (0, 4) else 4
        arrived(dxr.at[pl.ds(0, n), pl.ds(r0, rn), :], dd_s.at[h], dd_r.at[h, part], dev_c)

    def zslot(direction, piece, s):
        return (direction * 2 + piece) * 4 + s

    def back_wait(h, s, piece):
        r0, rn = TOKS[h]
        n = sum(s >= 4 - HOPS[d][piece] for d in (0, 1))
        arrived(zr.at[pl.ds(0, n), pl.ds(r0, rn), :], dz_s.at[h], dz_r.at[h, s, piece], dev_z[0])

    def back_step(h, s):
        r0, rn = TOKS[h]
        core_wait(h, s)
        for piece in (0, 1):
            if s > 4 - max(HOPS[0][piece], HOPS[1][piece]):
                back_wait(h, s - 1, piece)
            for direction in (0, 1):
                first = 4 - HOPS[direction][piece]
                if s < first:
                    continue
                k = 4 - s if direction == 0 else 4 + s
                v = core_sum(h, piece, k)
                if s > first:
                    v = v + zr[zslot(direction, piece, s - 1), r0:r0 + rn, :].astype(F32)
                i = zslot(direction, piece, s)
                zs[i, r0:r0 + rn, :] = v.astype(BF)
                send(zs.at[i, pl.ds(r0, rn), :], zr.at[i, pl.ds(r0, rn), :], dz_s.at[h], dz_r.at[h, s, piece],
                     dev_z[direction])

    def back_last(h):
        r0, rn = TOKS[h]
        rows = pl.ds(r0, rn)
        core_wait(h, 4)
        for piece in (0, 1):
            back_wait(h, 3, piece)
            v = core_sum(h, piece, 0)
            for direction in (0, 1):
                v = v + zr[zslot(direction, piece, 3), r0:r0 + rn, :].astype(F32)
            fs[piece, r0:r0 + rn, :] = v.astype(BF)
            if piece == 0:
                @pl.when(away)
                def _():
                    send(fs.at[0, rows, :], fr.at[0, rows, :], f_s.at[0], f_r.at[h, 0], dev_p)

                @pl.when(jnp.logical_not(away))
                def _():
                    fr[0, r0:r0 + rn, :] = fs[0, r0:r0 + rn, :]
            else:
                send(fs.at[1, rows, :], fr.at[1, rows, :], f_s.at[1], f_r.at[h, 1], dev_s2)

    def back_out(h):
        r0, rn = TOKS[h]
        rows = pl.ds(r0, rn)

        @pl.when(away)
        def _():
            arrived(fr.at[0, rows, :], f_s.at[0], f_r.at[h, 0], dev_p)

        arrived(fr.at[1, rows, :], f_s.at[1], f_r.at[h, 1], dev_d2)
        ig[r0:r0 + rn, :] = (fr[0, r0:r0 + rn, :].astype(F32) + fr[1, r0:r0 + rn, :].astype(F32)).astype(BF)

    tok_scatter(0)
    tok_scatter(1)
    w_here(0)
    w_send(0)
    w_here(1)
    w_send(1)
    w_here(2)
    w_send(2)
    w_here(3)
    w_send(3)
    blend(0, True)
    blend(1, True)
    blend(2, True)
    blend(3, True)
    tok_step(0, 0)
    tok_step(1, 0)
    tok_step(0, 1)
    tok_step(0, 2)
    w_arrive(0)
    tok_step(1, 1)
    tok_step(0, 3)
    blend(0, False)
    tok_step(1, 2)
    tok_step(0, 4)
    tok_done(0)
    forward(0)
    tok_step(1, 3)
    reduce(0)
    w_arrive(1)
    tok_step(1, 4)
    blend(1, False)
    forward(2)
    tok_done(1)
    forward(5)
    forward(1)
    hg_load.wait()
    middle(0)
    reduce(2)
    reduce(5)
    reduce(1)
    spread(0)
    w_arrive(2)
    blend(2, False)
    forward(3)
    forward(6)
    middle(2)
    reduce(3)
    w_arrive(3)
    blend(3, False)
    forward(4)
    forward(7)
    reduce(6)
    reduce(4)
    gathered(0)
    turn(0)
    reduce(7)
    middle(3)
    middle(4)
    middle(7)
    spread(2)
    spread(3)
    spread(4)
    middle(5)
    middle(6)
    gathered(2)
    turn(2)
    middle(1)
    hid_copy.start()
    gathered(3)
    turn(3)
    gathered(4)
    turn(4)
    spread(7)
    back(0, 0)
    back(0, 1)
    back_step(0, 0)
    back(0, 2)
    back(0, 4)
    spread(5)
    back_step(0, 1)
    spread(6)
    spread(1)
    back(0, 3)
    gathered(5)
    turn(5)
    gathered(7)
    turn(7)
    back_step(0, 2)
    gathered(6)
    turn(6)
    gathered(1)
    turn(1)
    back(1, 0)
    back_step(1, 0)
    bend(2)
    back(1, 1)
    back_step(0, 3)
    back_step(1, 1)
    bend(0)
    back(1, 2)
    back_last(0)
    back_step(1, 2)
    bend(1)
    back(1, 3)
    bend(3)
    back(1, 4)
    back_step(1, 3)
    back_last(1)
    bend_out(2)
    bend_out(0)
    back_out(0)
    bend_out(1)
    bend_out(3)
    back_out(1)
    ig_copy.start()

    hid_copy.wait()
    pltpu.make_async_copy(dw, dw, o_s.at[2]).wait()

    @pl.when(away)
    def _():
        left(tokt, p0_s.at[0], p0_r.at[0, 0], dev_p)
        left(fs.at[0], f_s.at[0], f_r.at[0, 0], dev_p)

    left(tokt, p0_s.at[1], p0_r.at[0, 1], dev_d2)
    left(fs.at[1], f_s.at[1], f_r.at[0, 1], dev_s2)
    left(raw, w_s.at[0], w_r.at[0], dev_y)
    left(ysend, y_s.at[0], y_r.at[0], dev_y)
    left(fbuf.at[pl.ds(0, 3)], x_s.at[0], x_r.at[0, 0], dev_xp)
    for h in range(NH):
        r0, rn = TOKS[h]
        rows = pl.ds(r0, rn)
        left(zs.at[pl.ds(0, 14), rows, :], tz_s.at[h], tz_r.at[h, 0, 0], dev_z[0])
        left(zs.at[pl.ds(0, 14), rows, :], dz_s.at[h], dz_r.at[h, 0, 0], dev_z[0])
        left(dxs.at[:, rows, :], td_s.at[h], td_r.at[h], dev_c)
        left(dxs.at[:, rows, :], dd_s.at[h], dd_r.at[h, 0], dev_c)
    ig_copy.wait()


def hand_on(*refs):
    srcs, dsts, held = refs[0:4], refs[4:8], refs[8:12]
    s_in, s_out = refs[12], refs[13]
    ins = [pltpu.make_async_copy(srcs[i], held[i], s_in.at[i]) for i in range(4)]
    outs = [pltpu.make_async_copy(held[i], dsts[i], s_out.at[i]) for i in range(4)]
    for i in range(4):
        ins[i].start()
    for i in range(4):
        ins[i].wait()
        outs[i].start()
    for i in range(4):
        outs[i].wait()


def per_device(tokens, t_values, *rest):
    a = pl.BlockSpec(memory_space=pl.ANY)
    dma = pltpu.SemaphoreType.DMA
    vm = pltpu.VMEM
    scratch = [
        pltpu.SMEM((8,), F32),
        vm((512, 128), BF),
        vm((128, 512), BF),
        vm((3, 896, 512), BF),
        vm((3, 896, 512), BF),
        vm((448, 512), BF),
        vm((448, 512), BF),
        vm((512, 128), BF),
        vm((4, 1024, 512), BF),
        vm((4, 896, 1024), BF),
        vm((4, 896, 512), F32),
        vm((3, 896, 512), BF),
        vm((896, 512), BF),
        vm((2, 896, 512), BF),
        vm((4, 896, 512), BF),
        vm((4, 512, 896), BF),
        vm((896, 512), F32),
        vm((896, 512), BF),
        vm((896, 512), BF),
        vm((16, 512, 128), F32),
        vm((16, 512, 128), BF),
        vm((16, 512, 128), BF),
        vm((16, 512, 128), BF),
        vm((16, 512, 128), BF),
        vm((2, 512, 128), BF),
        vm((2, 512, 128), BF),
        dma((3 + NF,)),
        dma((3,)),
    ]
    for out, into in (((2,), (NH, 2)), ((NH,), (NH, 4, 2)), ((NH,), (NH,)), ((1,), (NF,)), ((1,), (NC, 4)),
                      ((1,), (NF,)), ((NH,), (NH, 5)), ((NH,), (NH, 4, 2)), ((2,), (NH, 2))):
        scratch += [dma(out), dma(into)]
    shapes = (
        jax.ShapeDtypeStruct((448, 512), BF),
        jax.ShapeDtypeStruct((512, 128), BF),
        jax.ShapeDtypeStruct((448, 512), F32),
        jax.ShapeDtypeStruct((448, 512), F32),
    )
    results = pl.pallas_call(
        kernel,
        out_shape=shapes,
        in_specs=[a] * 9,
        out_specs=(a, a, a, a),
        scratch_shapes=scratch,
        compiler_params=pltpu.CompilerParams(
            collective_id=0, has_side_effects=True, vmem_limit_bytes=67_043_328
        ),
    )(tokens, t_values, *(w.T for w in rest))
    hidden, input_grad, gate_grad, up_grad = pl.pallas_call(
        hand_on,
        out_shape=shapes,
        in_specs=[a] * 4,
        out_specs=(a, a, a, a),
        scratch_shapes=[vm(v.shape, v.dtype) for v in shapes] + [dma((4,)), dma((4,))],
    )(*results)
    return hidden.T, input_grad, gate_grad.T, up_grad.T


def solution(mesh):
    return jax.shard_map(
        per_device,
        mesh=mesh,
        in_specs=(P("pt", "tp"), P()) + (P("pt", "tp"),) * 7,
        out_specs=(P("pt", "tp"),) * 4,
        check_vma=False,
    )
```
